256 devices in a mesh: rep: 128 (over x, z, y_hi, core), dom: 2 (over y_lo).
Axes of the slice: x: 4, y: 4 (y_hi: 2, y_lo: 2; y = y_hi * 2 + y_lo), z: 8, core: 2. Of those that a mesh axis runs over, the one named last changes fastest.
Arguments:
- field: float32 [128, 256, 2048], P('rep', 'dom'), may hold values from -2.5 to 2.5
- momentum: float32 [128, 256, 2048], P('rep', 'dom'), may hold values from -4 to 4
- labels: int32 [128], P('rep'), may hold values from 0 to 127, each once
- betas: float32 [128], replicated, may hold values from 0.4 to 1.6
- accept: int32 [128], P('rep'), may hold values 0 or 1
- swap_pairs: int32 [128], replicated, may hold values from 0 to 127, as said below
Outputs:
- field_out: float32 [128, 256, 2048], P('rep', 'dom')
- field_sorted: float32 [128, 256, 2048], P('rep', 'dom')
- labels_out: int32 [128], P('rep')
- energy_change: float32 [128], P('rep')
- ladder_action: float32 [128], P('rep')
The draws below stay inside these ranges and needn't reach their ends.
Inputs may be any that keep to these rules, and one draw needn't show every extreme that they name: Each temperature index t is paired with itself, with t - 1 or with t + 1, and the pairing is symmetric: swap_pairs[swap_pairs[t]] = t. labels is a permutation of the temperature indices.
All inputs are finite; a program needn't handle non-finite values. No bound on the sum of `accept` on one device may be relied on, other than what follows from the above.
Results may differ from the reference program's by a relative error of at most 0.0003.
Values sent between devices are 32-bit elements; how exact they have to be, the bound alone decides.
A program may use at most 64 MiB of HBM per device.

```python
import math
import jax
import jax.numpy as jnp
from jax import lax

COLS = 2048
STEPS = 8
REPLICAS = 128
ROWS = 256


def draw_swap_pairs(key, part):
    key_parity = jax.random.fold_in(key, 11)
    key_accept = jax.random.fold_in(key, 12)
    parity = jax.random.randint(key_parity, (), 0, 2)
    positions = jnp.arange(REPLICAS, dtype=jnp.int32)
    offset = (positions - parity) % 2
    candidate = jnp.where(offset == 0, positions + 1, positions - 1)
    inside = (candidate >= 0) & (candidate < REPLICAS)
    flips = jax.random.randint(key_accept, (REPLICAS,), 0, 2)
    lower_end = jnp.clip(jnp.minimum(positions, candidate), 0, REPLICAS - 1)
    agreed = jnp.take(flips, lower_end) == 1
    return jnp.where(inside & agreed, candidate, positions).astype(jnp.int32)


def place_ends(values, stream_key, smallest, top_value):
    shape = values.shape
    spot = [jax.random.randint(jax.random.fold_in(stream_key, axis), (), 0, shape[axis]) for axis in range(len(shape))]
    values = values.at[tuple(spot)].set(smallest)
    longest = shape.index(max(shape))
    spot[longest] = (spot[longest] + 1) % shape[longest]
    return values.at[tuple(spot)].set(top_value)


def levels(rng, extent, cuts, smallest, top_value):
    def one(position, blocks):
        draws = jax.random.uniform(jax.random.fold_in(jax.random.fold_in(rng, 6), position), (blocks,), jnp.float32, smallest / len(cuts), top_value / len(cuts))
        return jnp.repeat(jnp.exp(draws), extent[position] // blocks).reshape((-1,) + (1,) * (len(extent) - position - 1))

    level = one(*cuts[0])
    for cut in cuts[1:]:
        level = level * one(*cut)
    return level


def noise(key, extent, deviation, most, pieces=(), held_as=jnp.bfloat16):
    entries = jax.random.normal(key, extent, jnp.float32) * deviation
    if len(pieces) > 0:
        entries = levels(key, extent, pieces, -0.22, 0.18) * entries
    return jnp.clip(entries, min=-most, max=most).astype(held_as)


def setup_inputs(seed: int = 0) -> dict:
    keys = jax.random.split(jax.random.key(seed), 7)
    return {
        "field": noise(keys[0], (REPLICAS, ROWS, COLS), 0.7, 2.5, ((0, 128), (1, 2)), jnp.float32),
        "momentum": noise(keys[1], (REPLICAS, ROWS, COLS), 1.0, 4.0, ((0, 128), (1, 2)), jnp.float32),
        "labels": jax.random.permutation(keys[2], REPLICAS).astype(jnp.int32),
        "betas": jnp.clip(jnp.exp(jax.random.uniform(keys[3], (REPLICAS,), jnp.float32, math.log(0.4), math.log(1.6))), 0.4, 1.6),
        "accept": place_ends((jax.random.randint(keys[4], (REPLICAS,), 0, 4) < 3).astype(jnp.int32), jax.random.fold_in(keys[4], 1), 0, 1),
        "swap_pairs": draw_swap_pairs(jax.random.fold_in(keys[6], 71), 0),
    }


hopping = 0.18
quartic = 0.3
step_size = 0.05


def force_field(values, coldness):
    beside_all = (jnp.roll(values, 1, 0) + jnp.roll(values, -1, 0)) + (jnp.roll(values, 1, 1) + jnp.roll(values, -1, 1))
    return coldness * (-2.0 * hopping * beside_all + 2.0 * values + 4.0 * quartic * values * (values * values - 1.0))


def site_action(values):
    neighbours = jnp.roll(values, -1, 0) + jnp.roll(values, -1, 1)
    squared = values * values
    return -2.0 * hopping * values * neighbours + squared + quartic * (squared - 1.0) * (squared - 1.0)


def trajectory(inputs):
    start_field, start_moment, coldness = inputs
    moment = start_moment - 0.5 * step_size * force_field(start_field, coldness)
    current = start_field
    for leap_step in range(STEPS):
        current = current + step_size * moment
        factor = 0.5 * step_size if leap_step == STEPS - 1 else step_size
        moment = moment - factor * force_field(current, coldness)
    old_action = site_action(start_field)
    new_action = site_action(current)
    change = jnp.sum((0.5 * moment * moment + coldness * new_action) - (0.5 * start_moment * start_moment + coldness * old_action))
    return current, change, jnp.sum(old_action), jnp.sum(new_action)


def reference(field, momentum, labels, betas, accept, swap_pairs):
    coldness = betas[labels]
    labels_out = swap_pairs[labels]
    proposal, change, old_total, new_total = lax.map(trajectory, (field, momentum, coldness))
    accepted = accept == 1
    field_out = jnp.where(accepted[:, None, None], proposal, field)
    action = jnp.where(accepted, new_total, old_total)
    holder = jnp.zeros((REPLICAS,), jnp.int32).at[labels_out].set(jnp.arange(REPLICAS, dtype=jnp.int32))
    field_sorted = field_out[holder]
    ladder_action = action[holder] / (ROWS * COLS)
    return field_out, field_sorted, labels_out, change, ladder_action
```

```python
import functools
import jax
import jax.numpy as jnp
from jax import lax
from jax.experimental import pallas as pl
from jax.experimental.pallas import tpu as pltpu
from jax.sharding import PartitionSpec as P

STEPS = 8
MESH = pl.DeviceIdType.MESH

hopping = 0.18
quartic = 0.3
step_size = 0.05

def with_halo(cells, sides, width):
    for axis, dim in sides:
        count = lax.axis_size(axis)
        head = lax.slice_in_dim(cells, 0, width, axis=dim)
        tail = lax.slice_in_dim(cells, cells.shape[dim] - width, cells.shape[dim], axis=dim)
        cells = jnp.concatenate(
            [
                lax.ppermute(tail, axis, [(i, (i + 1) % count) for i in range(count)]),
                cells,
                lax.ppermute(head, axis, [((i + 1) % count, i) for i in range(count)]),
            ],
            axis=dim,
        )
    return cells


def force_rows(padded, coldness):
    centre = padded[1:-1]
    beside_all = padded[:-2] + padded[2:] + (jnp.roll(centre, 1, 1) + jnp.roll(centre, -1, 1))
    return coldness * (
        -2.0 * hopping * beside_all
        + 2.0 * centre
        + 4.0 * quartic * centre * (centre * centre - 1.0)
    )


def site_terms(padded, margin, strip_rows):
    values = padded[margin : margin + strip_rows]
    lower_row = padded[margin + 1 : margin + 1 + strip_rows]
    neighbours = lower_row + jnp.roll(values, -1, 1)
    squared = values * values
    return (
        -2.0 * hopping * values * neighbours + squared + quartic * (squared - 1.0) * (squared - 1.0)
    )


def trim_rows(values, margin, target):
    excess = margin - target
    return values[excess : values.shape[0] - excess]


def split_rep(rep):
    return rep // 32, (rep // 4) % 8, (rep // 2) % 2, rep % 2


def join_rep(x, z, y, c):
    return ((x * 8 + z) * 2 + y) * 2 + c


def table_place(rep):
    x, z, y, c = split_rep(rep)
    return ((x * 2 + y) * 2 + c) * 8 + z


def tile_of(ref, chunk, home):
    block = lax.rem(4 + 8 * chunk + lax.div(home, 16), 16)
    rows = pl.ds(pl.multiple_of(block * 8, 8), 8)
    cols = pl.ds(pl.multiple_of(lax.rem(home, 16) * 128, 128), 128)
    return ref.at[0, rows, cols]


def wait_for(ref, sem):
    pltpu.make_async_copy(ref, ref, sem).wait()


def exchange(
    field_ref, info_ref, label_ref,
    sorted_ref, change_ref, ladder_ref,
    got_0, got_1, picked, label_row, label_tab, act_row, act_got, act_sum, act_tab, holder_row, holder_ref,
    send_1, recv_1, send_2, recv_2, send_lab, recv_lab, send_act, recv_act, local_sem,
):
    me = lax.axis_index("rep")
    dom = lax.axis_index("dom")
    other = 1 - dom
    x, z, y, c = split_rep(me)
    place = table_place(me)
    group = lax.div(place, 8)
    got = (got_0, got_1)

    def push(src, dst, send_sem, recv_sem, rep):
        pltpu.make_async_remote_copy(
            src_ref=src, dst_ref=dst, send_sem=send_sem, recv_sem=recv_sem,
            device_id=(rep, other), device_id_type=MESH,
        ).start()

    barrier = pltpu.get_barrier_semaphore()

    def greet(k, carry):
        pl.semaphore_signal(barrier, inc=1, device_id=(lax.rem(me + k, 128), other), device_id_type=MESH)
        return carry

    lax.fori_loop(0, 128, greet, 0)

    def to_column(row, tab, send_sem, recv_sem):
        for k in range(8):
            push(row, tab.at[place], send_sem, recv_sem, join_rep(x, (z + k) % 8, y, c))

    def to_plane(tab, out, send_sem, recv_sem):
        block = pl.ds(pl.multiple_of(group * 8, 8), 8)
        for k in range(16):
            push(
                tab.at[block], out.at[block], send_sem, recv_sem,
                join_rep((x + k // 4) % 4, z, (y + (k // 2) % 2) % 2, (c + k % 2) % 2),
            )

    def spread(chunk):
        def one(k, carry):
            home = lax.rem(me + k, 128)
            push(tile_of(field_ref, chunk, home), got[chunk].at[me], send_1.at[chunk], recv_1.at[chunk], home)
            return carry

        lax.fori_loop(0, 128, one, 0)

    def gather(chunk):
        def pick(t, carry):
            picked[chunk, t] = got[chunk][holder_ref[0, t]]
            return carry

        lax.fori_loop(0, 128, pick, 0, unroll=8)

        def one(k, carry):
            goal = lax.rem(me + k, 128)
            push(picked.at[chunk, goal], tile_of(sorted_ref, chunk, me), send_2.at[chunk], recv_2, goal)
            return carry

        lax.fori_loop(0, 128, one, 0)

    lane = lax.broadcasted_iota(jnp.int32, (1, 128), 1)
    label_row[...] = jnp.full((1, 128), label_ref[0], jnp.int32)
    act_row[...] = info_ref[...]
    pl.semaphore_wait(barrier, 128)

    to_column(label_row, label_tab.at[0], send_lab.at[0], recv_lab.at[0])
    push(act_row, act_got, send_act.at[0], recv_act.at[0], me)
    spread(0)
    wait_for(label_tab.at[0, pl.ds(0, 8)], recv_lab.at[0])
    to_plane(label_tab.at[0], label_tab.at[1], send_lab.at[1], recv_lab.at[1])
    wait_for(act_got, recv_act.at[0])
    total = act_row[...] + act_got[...]
    act_sum[...] = total
    to_column(act_sum, act_tab.at[0], send_act.at[1], recv_act.at[1])
    spread(1)

    wait_for(label_tab.at[1], recv_lab.at[1])
    holder = jnp.zeros((1, 128), jnp.int32)
    for p in range(128):
        rep = join_rep(p // 32, p % 8, (p // 16) % 2, (p // 8) % 2)
        holder = jnp.maximum(holder, jnp.where(label_tab[1, p] == lane, rep, 0))
    holder_row[...] = holder
    copy = pltpu.make_async_copy(holder_row, holder_ref, local_sem)
    copy.start()
    copy.wait()

    wait_for(act_tab.at[0, pl.ds(0, 8)], recv_act.at[1])
    to_plane(act_tab.at[0], act_tab.at[1], send_act.at[2], recv_act.at[2])
    wait_for(got_0, recv_1.at[0])
    gather(0)
    wait_for(got_1, recv_1.at[1])
    gather(1)

    wait_for(act_tab.at[1], recv_act.at[2])
    ladder = jnp.zeros((1, 128), jnp.float32)
    for p in range(128):
        ladder = ladder + jnp.where(label_tab[1, p] == me, act_tab[1, p], 0.0)
    ladder_ref[0] = jnp.sum(jnp.where(lane == 0, ladder, 0.0)) / 524288.0
    change_ref[0] = jnp.sum(jnp.where(lane == 1, total, 0.0))

    wait_for(label_tab.at[0, pl.ds(0, 8)], send_lab.at[0])
    wait_for(label_tab.at[1], send_lab.at[1])
    wait_for(act_got, send_act.at[0])
    wait_for(act_tab.at[0, pl.ds(0, 8)], send_act.at[1])
    wait_for(act_tab.at[1], send_act.at[2])
    for chunk in range(2):
        wait_for(got[chunk], send_1.at[chunk])
        wait_for(got[chunk], send_2.at[chunk])
    wait_for(sorted_ref, recv_2)


def body(field, momentum, labels, betas, accept, swap_pairs):
    strip_rows = field.shape[1]
    ladder_index = jnp.arange(betas.shape[0], dtype=jnp.int32)
    chosen = ladder_index == labels[0]
    coldness = jnp.sum(jnp.where(chosen, betas, 0.0))
    new_label = jnp.sum(jnp.where(chosen, swap_pairs, 0))
    start_field = field[0]
    start_moment = momentum[0]
    current = start_field
    moment = start_moment
    margin = 0
    old_action = None
    new_action = None
    for leap_step in range(STEPS + 1):
        if margin == 0:
            stacked = with_halo(jnp.stack((current, moment)), (("dom", 1),), 3)
            current = stacked[0]
            moment = stacked[1]
            margin = 3
        padded = current
        outer = margin
        if leap_step == 0:
            old_action = site_terms(padded, outer, strip_rows)
        if leap_step == STEPS:
            new_action = site_terms(padded, outer, strip_rows)
        force_now = force_rows(padded, coldness)
        moment = trim_rows(moment, margin, outer - 1)
        current = trim_rows(padded, outer, outer - 1)
        margin = outer - 1
        factor = 0.5 * step_size if leap_step == 0 or leap_step == STEPS else step_size
        moment = moment - factor * force_now
        if leap_step < STEPS:
            current = current + step_size * moment
    change_part = jnp.sum(
        0.5 * moment * moment
        + coldness * new_action
        - (0.5 * start_moment * start_moment + coldness * old_action)
    )
    accepted = accept[0] == 1
    action_part = jnp.where(accepted, jnp.sum(new_action), jnp.sum(old_action))
    field_out = jnp.where(accepted, current, start_field)
    lane = jnp.arange(128)[None]
    info = jnp.where(lane == 0, action_part, jnp.where(lane == 1, change_part, 0.0))
    vmem = pl.BlockSpec(memory_space=pltpu.VMEM)
    smem = pl.BlockSpec(memory_space=pltpu.SMEM)
    f32, i32 = jnp.float32, jnp.int32
    dma = pltpu.SemaphoreType.DMA
    ordered, change, ladder = pl.pallas_call(
        exchange,
        out_shape=(
            jax.ShapeDtypeStruct((1, 128, 2048), f32),
            jax.ShapeDtypeStruct((1,), f32),
            jax.ShapeDtypeStruct((1,), f32),
        ),
        in_specs=[vmem, vmem, smem],
        out_specs=(vmem, smem, smem),
        scratch_shapes=[
            pltpu.VMEM((128, 8, 128), f32),
            pltpu.VMEM((128, 8, 128), f32),
            pltpu.VMEM((2, 128, 8, 128), f32),
            pltpu.VMEM((1, 128), i32),
            pltpu.VMEM((2, 128, 1, 128), i32),
            pltpu.VMEM((1, 128), f32),
            pltpu.VMEM((1, 128), f32),
            pltpu.VMEM((1, 128), f32),
            pltpu.VMEM((2, 128, 1, 128), f32),
            pltpu.VMEM((1, 128), i32),
            pltpu.SMEM((1, 128), i32),
            dma((2,)), dma((2,)), dma((2,)), dma(()), dma((2,)), dma((2,)), dma((3,)), dma((3,)), dma(()),
        ],
        compiler_params=pltpu.CompilerParams(collective_id=0, has_side_effects=True, vmem_limit_bytes=32 << 20),
    )(field_out[None], info, new_label[None])
    return (field_out[None], ordered, new_label[None], change, ladder)


def solution(mesh):
    rep = P("rep")
    strip = P("rep", "dom", None)
    in_specs = (strip, strip, rep, P(), rep, P())
    out_specs = (strip, strip, rep, rep, rep)
    return jax.shard_map(body, mesh=mesh, in_specs=in_specs, out_specs=out_specs, check_vma=False)
```

```python
import functools
import jax
import jax.numpy as jnp
from jax import lax
from jax.experimental import pallas as pl
from jax.experimental.pallas import tpu as pltpu
from jax.sharding import PartitionSpec as P

MESH = pl.DeviceIdType.MESH

HOP = 0.36
QUARTIC = 0.3
EPS = 0.05
F32 = jnp.float32
BF16 = jnp.bfloat16

def split_rep(rep):
    return rep // 32, (rep // 4) % 8, (rep // 2) % 2, rep % 2


def join_rep(x, z, y, c):
    return ((x * 8 + z) * 2 + y) * 2 + c


def table_place(rep):
    x, z, y, c = split_rep(rep)
    return ((x * 2 + y) * 2 + c) * 8 + z


def tile_of(ref, chunk, home):
    block = lax.rem(4 + 8 * chunk + lax.div(home, 16), 16)
    rows = pl.ds(pl.multiple_of(block * 8, 8), 8)
    cols = pl.ds(pl.multiple_of(lax.rem(home, 16) * 128, 128), 128)
    return ref.at[0, rows, cols]


def wait_for(ref, sem):
    pltpu.make_async_copy(ref, ref, sem).wait()


def rows_of(block):
    return pl.ds(pl.multiple_of(block * 8, 8), 8)


def lateral(q):
    even, odd = q[:, :1024], q[:, 1024:]
    after = pltpu.roll(even, 1023, 1)
    return jnp.concatenate((odd + pltpu.roll(odd, 1, 1), even + after), 1), jnp.concatenate((odd, after), 1)


def fold(v):
    total = v[:, :128]
    for j in range(1, 16):
        total = total + v[:, 128 * j : 128 * j + 128]
    return total


def split_two(v):
    high = v.astype(BF16)
    return high, (v - high.astype(F32)).astype(BF16)


def site(q, below, right):
    squared = q * q
    return -HOP * q * (below + right) + squared + QUARTIC * (squared - 1.0) * (squared - 1.0)


def whole(
    field_ref, moment_ref, labels_ref, betas_ref, accept_ref, pairs_ref,
    out_ref, sorted_ref, new_ref, change_ref, ladder_ref,
    q0, m0, qa, pa, qe, pe, perm, perm_back,
    got_0, got_1, picked, label_row, label_tab, act_row, act_got, act_sum, act_tab, holder_row, holder_ref,
    send_h, recv_h, send_1, recv_1, send_2, recv_2, send_lab, recv_lab, send_act, recv_act, local_sem,
):
    me = lax.axis_index("rep")
    dom = lax.axis_index("dom")
    other = 1 - dom
    x, z, y, c = split_rep(me)
    place = table_place(me)
    group = lax.div(place, 8)
    got = (got_0, got_1)

    def push(src, dst, send_sem, recv_sem, rep):
        pltpu.make_async_remote_copy(
            src_ref=src, dst_ref=dst, send_sem=send_sem, recv_sem=recv_sem,
            device_id=(rep, other), device_id_type=MESH,
        ).start()

    barrier = pltpu.get_barrier_semaphore()

    def greet(k, carry):
        pl.semaphore_signal(barrier, inc=1, device_id=(lax.rem(me + k, 128), other), device_id_type=MESH)
        return carry

    lax.fori_loop(0, 128, greet, 0, unroll=8)

    label = labels_ref[0]
    coldness = betas_ref[label]
    new_label = pairs_ref[label]
    accepted = accept_ref[0] == 1
    new_ref[0] = new_label
    label_row[...] = jnp.full((1, 128), new_label, jnp.int32)

    i0 = lax.broadcasted_iota(jnp.int32, (256, 256), 0)
    i1 = lax.broadcasted_iota(jnp.int32, (256, 256), 1)
    there = jnp.where(i1 < 128, 2 * i1, 2 * i1 - 255) == i0
    back = jnp.where(i0 < 128, 2 * i0, 2 * i0 - 255) == i1
    for third in range(3):
        perm[pl.ds(256 * third, 256), :] = jnp.where(there, 1.0, 0.0).astype(BF16)
    for half in range(2):
        perm_back[pl.ds(256 * half, 256), :] = jnp.where(back, 1.0, 0.0).astype(BF16)

    def apart(ref, dst, r):
        values = ref[0, pl.ds(pl.multiple_of(32 * r, 32), 32), :]
        high = values.astype(BF16)
        pieces = (high, *split_two(values - high.astype(F32)))
        cols = [slice(256 * b, 256 * b + 256) for b in range(8)]
        left = jnp.concatenate([jnp.concatenate([v[:, s] for v in pieces], 1) for s in cols], 0)
        res = jnp.dot(left, perm[...], preferred_element_type=F32)
        rows = pl.ds(pl.multiple_of(16 + 32 * r, 16), 32)
        for b in range(8):
            dst[rows, 128 * b : 128 * b + 128] = res[32 * b : 32 * b + 32, :128]
            dst[rows, 1024 + 128 * b : 1152 + 128 * b] = res[32 * b : 32 * b + 32, 128:]

    def joined(values):
        high, low = split_two(values)
        parts = []
        for b in range(8):
            e = slice(128 * b, 128 * b + 128)
            o = slice(1024 + 128 * b, 1152 + 128 * b)
            parts.append(jnp.concatenate((high[:, e], high[:, o], low[:, e], low[:, o]), 1))
        res = jnp.dot(jnp.concatenate(parts, 0), perm_back[...], preferred_element_type=F32)
        return jnp.concatenate([res[32 * b : 32 * b + 32] for b in range(8)], 1)

    def settle(values, rows):
        for at, n, first in rows:
            old = field_ref[0, pl.ds(first, n), :]
            out_ref[0, pl.ds(first, n), :] = jnp.where(accepted, values[at : at + n], old)

    def set_apart(r, carry):
        apart(field_ref, q0, r)
        apart(moment_ref, m0, r)
        return carry

    lax.fori_loop(0, 4, set_apart, 0)

    row = lax.broadcasted_iota(jnp.int32, (8, 2048), 0)
    a = coldness * (EPS * EPS * HOP)
    b = coldness * (EPS * EPS * (2.0 - 4.0 * QUARTIC))
    g = coldness * (EPS * EPS * 4.0 * QUARTIC)

    def around(ref, block):
        q = ref[rows_of(block), :]
        above = pltpu.roll(jnp.where(row == 7, ref[rows_of(block - 1), :], q), 1, 0)
        below = pltpu.roll(jnp.where(row == 0, ref[rows_of(block + 1), :], q), 7, 0)
        return q, above, below

    def kicked(q, above, below, beside, moment, share):
        near = (above + below) + beside
        return moment + (near * (share * a) - q * (q * q * (share * g) + share * b))

    def leap(src, src_at, mom, mom_at, dst, dst_p, at, first):
        q, above, below = around(src, src_at)
        beside, _ = lateral(q)
        moment = mom[rows_of(mom_at), :]
        moment = kicked(q, above, below, beside, moment * EPS if first else moment, 0.5 if first else 1.0)
        dst_p[rows_of(at), :] = moment
        dst[rows_of(at), :] = q + moment

    def finish(src, src_at, mom, mom_at, start_at, sums):
        q, above, below = around(src, src_at)
        beside, right = lateral(q)
        moment = kicked(q, above, below, beside, mom[rows_of(mom_at), :], 0.5)
        new = site(q, below, right)
        p, _, p_below = around(q0, start_at)
        old = site(p, p_below, lateral(p)[1])
        start = m0[rows_of(start_at), :]
        change = (moment * moment * (0.5 / (EPS * EPS)) + coldness * new) - (0.5 * start * start + coldness * old)
        return sums[0] + fold(change), sums[1] + fold(jnp.where(accepted, new, old))

    def inner_first(i, carry):
        leap(q0, i, m0, i, qa.at[0], pa, i, True)
        return carry

    lax.fori_loop(3, 17, inner_first, 0)

    def inner(s, carry):
        cur = lax.rem(s - 1, 2)

        def one(i, inside):
            leap(qa.at[cur], i, pa, i, qa.at[1 - cur], pa, i, False)
            return inside

        return lax.fori_loop(3, 17, one, carry)

    lax.fori_loop(1, 8, inner, 0)
    zero = jnp.zeros((8, 128), F32)
    for part in range(2):
        first = 32 + 32 * part
        settle(joined(qa[1, pl.ds(16 + first, 32), :]), [(0, 32, first)])

    def to_column(src, tab, send_sem, recv_sem):
        for k in range(8):
            push(src, tab.at[place], send_sem, recv_sem, join_rep(x, (z + k) % 8, y, c))

    def to_plane(tab, dst, send_sem, recv_sem):
        block = pl.ds(pl.multiple_of(group * 8, 8), 8)
        for k in range(16):
            push(
                tab.at[block], dst.at[block], send_sem, recv_sem,
                join_rep((x + k // 4) % 4, z, (y + (k // 2) % 2) % 2, (c + k % 2) % 2),
            )

    def spread(chunk):
        def one(k, carry):
            home = lax.rem(me + k, 128)
            push(tile_of(out_ref, chunk, home), got[chunk].at[me], send_1.at[chunk], recv_1.at[chunk], home)
            return carry

        lax.fori_loop(0, 128, one, 0, unroll=4)

    def gather(chunk):
        def pick(t, carry):
            picked[chunk, t] = got[chunk][holder_ref[0, t]]
            return carry

        lax.fori_loop(0, 128, pick, 0, unroll=8)

        def one(k, carry):
            goal = lax.rem(me + k, 128)
            push(picked.at[chunk, goal], tile_of(sorted_ref, chunk, me), send_2.at[chunk], recv_2, goal)
            return carry

        lax.fori_loop(0, 128, one, 0, unroll=4)

    halos = ((q0, 136, 8, 8), (q0, 16, 144, 8), (m0, 136, 8, 8), (m0, 16, 144, 8), (q0, 135, 7, 1), (q0, 24, 152, 1))
    pl.semaphore_wait(barrier, 128)
    to_column(label_row, label_tab.at[0], send_lab.at[0], recv_lab.at[0])
    for k, (ref, src_row, dst_row, n) in enumerate(halos):
        push(ref.at[pl.ds(src_row, n)], ref.at[pl.ds(dst_row, n)], send_h.at[k], recv_h.at[k], me)
    spread(0)
    wait_for(label_tab.at[0, pl.ds(0, 8)], recv_lab.at[0])
    to_plane(label_tab.at[0], label_tab.at[1], send_lab.at[1], recv_lab.at[1])

    def inner_last(i, sums):
        return finish(qa.at[1], i, pa, i, i, sums)

    sums = lax.fori_loop(4, 16, inner_last, (zero, zero))
    settle(
        joined(jnp.concatenate((qa[1, pl.ds(32, 16), :], qa[1, pl.ds(112, 16), :]), 0)),
        [(0, 16, 16), (16, 16, 96)],
    )
    for k, (ref, src_row, dst_row, n) in enumerate(halos):
        wait_for(ref.at[pl.ds(dst_row, n)], recv_h.at[k])

    def outer_first(i, carry):
        side, local = lax.div(i, 4), 1 + lax.rem(i, 4)
        leap(q0, 14 * side + local, m0, 14 * side + local, qe.at[0], pe, 6 * side + local, True)
        return carry

    lax.fori_loop(0, 8, outer_first, 0)

    def outer(s, carry):
        cur = lax.rem(s - 1, 2)

        def one(i, inside):
            at = 6 * lax.div(i, 4) + 1 + lax.rem(i, 4)
            leap(qe.at[cur], at, pe, at, qe.at[1 - cur], pe, at, False)
            return inside

        return lax.fori_loop(0, 8, one, carry)

    lax.fori_loop(1, 8, outer, 0)
    settle(
        joined(jnp.concatenate((qe[1, pl.ds(16, 16), :], qe[1, pl.ds(64, 16), :]), 0)),
        [(0, 16, 0), (16, 16, 112)],
    )
    spread(1)

    def outer_last(i, sums):
        side, local = lax.div(i, 2), 2 + lax.rem(i, 2)
        return finish(qe.at[1], 6 * side + local, pe, 6 * side + local, 14 * side + local, sums)

    sums = lax.fori_loop(0, 4, outer_last, sums)
    lane = lax.broadcasted_iota(jnp.int32, (1, 128), 1)
    act_row[...] = jnp.where(lane == 0, jnp.sum(sums[1]), jnp.where(lane == 1, jnp.sum(sums[0]), 0.0))
    push(act_row, act_got, send_act.at[0], recv_act.at[0], me)

    wait_for(label_tab.at[1], recv_lab.at[1])
    holder = jnp.zeros((1, 128), jnp.int32)
    for p in range(128):
        rep = join_rep(p // 32, p % 8, (p // 16) % 2, (p // 8) % 2)
        holder = jnp.maximum(holder, jnp.where(label_tab[1, p] == lane, rep, 0))
    holder_row[...] = holder
    copy = pltpu.make_async_copy(holder_row, holder_ref, local_sem)
    copy.start()
    copy.wait()

    wait_for(got_0, recv_1.at[0])
    gather(0)
    wait_for(act_got, recv_act.at[0])
    total = act_row[...] + act_got[...]
    act_sum[...] = total
    to_column(act_sum, act_tab.at[0], send_act.at[1], recv_act.at[1])
    wait_for(got_1, recv_1.at[1])
    gather(1)
    wait_for(act_tab.at[0, pl.ds(0, 8)], recv_act.at[1])
    to_plane(act_tab.at[0], act_tab.at[1], send_act.at[2], recv_act.at[2])

    for k, (ref, src_row, dst_row, n) in enumerate(halos):
        wait_for(ref.at[pl.ds(src_row, n)], send_h.at[k])
    wait_for(label_tab.at[0, pl.ds(0, 8)], send_lab.at[0])
    wait_for(label_tab.at[1], send_lab.at[1])
    wait_for(act_got, send_act.at[0])
    wait_for(act_tab.at[0, pl.ds(0, 8)], send_act.at[1])
    for chunk in range(2):
        wait_for(got[chunk], send_1.at[chunk])
    change_ref[0] = jnp.sum(jnp.where(lane == 1, total, 0.0))
    wait_for(act_tab.at[1], recv_act.at[2])
    ladder = jnp.zeros((1, 128), F32)
    for p in range(128):
        ladder = ladder + jnp.where(label_tab[1, p] == me, act_tab[1, p], 0.0)
    ladder_ref[0] = jnp.sum(jnp.where(lane == 0, ladder, 0.0)) / 524288.0
    wait_for(act_tab.at[1], send_act.at[2])
    for chunk in range(2):
        wait_for(got[chunk], send_2.at[chunk])
    wait_for(sorted_ref, recv_2)


def body(field, momentum, labels, betas, accept, swap_pairs):
    vmem = pl.BlockSpec(memory_space=pltpu.VMEM)
    smem = pl.BlockSpec(memory_space=pltpu.SMEM)
    i32 = jnp.int32
    dma = pltpu.SemaphoreType.DMA
    strip = jax.ShapeDtypeStruct((1, 128, 2048), F32)
    out, ordered, new_label, change, ladder = pl.pallas_call(
        whole,
        out_shape=(
            strip, strip, jax.ShapeDtypeStruct((1,), i32),
            jax.ShapeDtypeStruct((1,), F32), jax.ShapeDtypeStruct((1,), F32),
        ),
        in_specs=[vmem, vmem, smem, smem, smem, smem],
        out_specs=(vmem, vmem, smem, smem, smem),
        scratch_shapes=[
            pltpu.VMEM((160, 2048), F32),
            pltpu.VMEM((160, 2048), F32),
            pltpu.VMEM((2, 160, 2048), F32),
            pltpu.VMEM((160, 2048), F32),
            pltpu.VMEM((2, 96, 2048), F32),
            pltpu.VMEM((96, 2048), F32),
            pltpu.VMEM((768, 256), BF16),
            pltpu.VMEM((512, 256), BF16),
            pltpu.VMEM((128, 8, 128), F32),
            pltpu.VMEM((128, 8, 128), F32),
            pltpu.VMEM((2, 128, 8, 128), F32),
            pltpu.VMEM((1, 128), i32),
            pltpu.VMEM((2, 128, 1, 128), i32),
            pltpu.VMEM((1, 128), F32),
            pltpu.VMEM((1, 128), F32),
            pltpu.VMEM((1, 128), F32),
            pltpu.VMEM((2, 128, 1, 128), F32),
            pltpu.VMEM((1, 128), i32),
            pltpu.SMEM((1, 128), i32),
            dma((6,)), dma((6,)), dma((2,)), dma((2,)), dma((2,)), dma(()),
            dma((2,)), dma((2,)), dma((3,)), dma((3,)), dma(()),
        ],
        compiler_params=pltpu.CompilerParams(collective_id=0, has_side_effects=True, vmem_limit_bytes=48 << 20),
    )(field, momentum, labels, betas, accept, swap_pairs)
    return out, ordered, new_label, change, ladder


def solution(mesh):
    rep = P("rep")
    strip = P("rep", "dom", None)
    in_specs = (strip, strip, rep, P(), rep, P())
    out_specs = (strip, strip, rep, rep, rep)
    return jax.shard_map(body, mesh=mesh, in_specs=in_specs, out_specs=out_specs, check_vma=False)
```

```python
import functools
import jax
import jax.numpy as jnp
from jax import lax
from jax.experimental import pallas as pl
from jax.experimental.pallas import tpu as pltpu
from jax.sharding import PartitionSpec as P

MESH = pl.DeviceIdType.MESH

HOP = 0.36
QUARTIC = 0.3
EPS = 0.05
F32 = jnp.float32
BF16 = jnp.bfloat16

def split_rep(rep):
    return rep // 32, (rep // 4) % 8, (rep // 2) % 2, rep % 2


def join_rep(x, z, y, c):
    return ((x * 8 + z) * 2 + y) * 2 + c


def table_place(rep):
    x, z, y, c = split_rep(rep)
    return ((x * 2 + y) * 2 + c) * 8 + z


def tile_of(ref, chunk, home):
    cols = pl.ds(pl.multiple_of(lax.rem(home, 16) * 128, 128), 128)
    if chunk == 0:
        return ref.at[4 + lax.div(home, 16), :, cols]
    b = lax.div(home, 32)
    block = 2 + b + 8 * lax.div(b, 2) if chunk == 1 else b + 12 * lax.div(b, 2)
    half = pl.ds(pl.multiple_of(4 * lax.rem(lax.div(home, 16), 2), 4), 4)
    return ref.at[block, half, cols]


def wait_for(ref, sem):
    pltpu.make_async_copy(ref, ref, sem).wait()


def rows_of(block):
    return pl.ds(pl.multiple_of(block * 8, 8), 8)


def lateral(q):
    even, odd = q[:, :1024], q[:, 1024:]
    after = pltpu.roll(even, 1023, 1)
    return jnp.concatenate((odd + pltpu.roll(odd, 1, 1), even + after), 1), jnp.concatenate((odd, after), 1)


def fold(v):
    total = v[:, :128]
    for j in range(1, 16):
        total = total + v[:, 128 * j : 128 * j + 128]
    return total


def split_two(v):
    high = v.astype(BF16)
    return high, (v - high.astype(F32)).astype(BF16)


def site(q, below, right):
    squared = q * q
    return -HOP * q * (below + right) + squared + QUARTIC * (squared - 1.0) * (squared - 1.0)


def whole(
    field_hbm, moment_hbm, labels_hbm, betas_hbm, accept_hbm, pairs_hbm,
    out_hbm, sorted_ref, new_hbm, change_hbm, ladder_hbm,
    labels_ref, betas_ref, accept_ref, pairs_ref, new_ref, change_ref, ladder_ref, out_ref,
    field_ref, moment_ref, q0, m0, qa_0, qa_1, pa, qe_0, qe_1, pe, perm, perm_back,
    got_0, got_1, got_2, picked_0, picked_1, picked_2, label_row, label_tab, act_row, act_got, act_sum, act_tab, holder_row, holder_ref,
    send_h, recv_h, send_1, recv_1, send_2, recv_2, send_lab, recv_lab, send_act, recv_act, local_sem, load_sem, small_sem, store_sem,
):
    me = lax.axis_index("rep")
    dom = lax.axis_index("dom")
    other = 1 - dom
    x, z, y, c = split_rep(me)
    place = table_place(me)
    group = lax.div(place, 8)
    got = (got_0, got_1, got_2)
    picked = (picked_0, picked_1, picked_2)

    loads = []
    for k, (src, dst) in enumerate(((field_hbm, field_ref), (moment_hbm, moment_ref))):
        loads.append(pltpu.make_async_copy(src.at[0], dst, load_sem.at[k]))
        loads[k].start()
    small = []
    for k, (src, dst) in enumerate(
        ((labels_hbm, labels_ref), (betas_hbm, betas_ref), (accept_hbm, accept_ref), (pairs_hbm, pairs_ref))
    ):
        small.append(pltpu.make_async_copy(src, dst, small_sem.at[k]))
        small[k].start()

    def push(src, dst, send_sem, recv_sem, rep):
        pltpu.make_async_remote_copy(
            src_ref=src, dst_ref=dst, send_sem=send_sem, recv_sem=recv_sem,
            device_id=(rep, other), device_id_type=MESH,
        ).start()

    barrier = pltpu.get_barrier_semaphore()

    xs = [lax.rem(x + k, 4) * 32 for k in (2, 1, 3, 0)]
    zs = [lax.rem(z + k, 8) * 4 for k in (4, 3, 5, 2, 6, 1, 7, 0)]
    for at_z in zs:
        for at_x in xs:
            for k in range(4):
                pl.semaphore_signal(barrier, inc=1, device_id=(at_x + at_z + k, other), device_id_type=MESH)

    for copy in small:
        copy.wait()
    label = labels_ref[0]
    coldness = betas_ref[label]
    new_label = pairs_ref[label]
    accepted = accept_ref[0] == 1
    new_ref[0] = new_label
    stores = [pltpu.make_async_copy(new_ref, new_hbm, store_sem.at[0])]
    stores[0].start()
    label_row[...] = jnp.full((1, 128), new_label, jnp.int32)

    i0 = lax.broadcasted_iota(jnp.int32, (256, 256), 0)
    i1 = lax.broadcasted_iota(jnp.int32, (256, 256), 1)
    there = jnp.where(i1 < 128, 2 * i1, 2 * i1 - 255) == i0
    back = jnp.where(i0 < 128, 2 * i0, 2 * i0 - 255) == i1
    for third in range(3):
        perm[pl.ds(256 * third, 256), :] = jnp.where(there, 1.0, 0.0).astype(BF16)
    for half in range(2):
        perm_back[pl.ds(256 * half, 256), :] = jnp.where(back, 1.0, 0.0).astype(BF16)

    def apart(ref, dst, r):
        values = ref[pl.ds(pl.multiple_of(32 * r, 32), 32), :]
        high = values.astype(BF16)
        pieces = (high, *split_two(values - high.astype(F32)))
        cols = [slice(256 * b, 256 * b + 256) for b in range(8)]
        left = jnp.concatenate([jnp.concatenate([v[:, s] for v in pieces], 1) for s in cols], 0)
        res = jnp.dot(left, perm[...], preferred_element_type=F32)
        rows = pl.ds(pl.multiple_of(16 + 32 * r, 16), 32)
        for b in range(8):
            dst[rows, 128 * b : 128 * b + 128] = res[32 * b : 32 * b + 32, :128]
            dst[rows, 1024 + 128 * b : 1152 + 128 * b] = res[32 * b : 32 * b + 32, 128:]

    def joined(values):
        high, low = split_two(values)
        parts = []
        for b in range(8):
            e = slice(128 * b, 128 * b + 128)
            o = slice(1024 + 128 * b, 1152 + 128 * b)
            parts.append(jnp.concatenate((high[:, e], high[:, o], low[:, e], low[:, o]), 1))
        res = jnp.dot(jnp.concatenate(parts, 0), perm_back[...], preferred_element_type=F32)
        return jnp.concatenate([res[32 * b : 32 * b + 32] for b in range(8)], 1)

    def settle(values, rows):
        for at, n, first in rows:
            new = jnp.where(accepted, values[at : at + n], field_ref[pl.ds(first, n), :])
            out_ref[pl.ds(first // 8, n // 8)] = new.reshape(n // 8, 8, 2048)

    for load, ref, dst in zip(loads, (field_ref, moment_ref), (q0, m0)):
        load.wait()

        def set_apart(r, carry, ref=ref, dst=dst):
            apart(ref, dst, r)
            return carry

        lax.fori_loop(0, 4, set_apart, 0)

    row = lax.broadcasted_iota(jnp.int32, (8, 2048), 0)
    a = coldness * (EPS * HOP)
    b = coldness * (EPS * (2.0 - 4.0 * QUARTIC))
    g = coldness * (EPS * 4.0 * QUARTIC)

    def around(ref, block):
        q = ref[rows_of(block), :]
        above = pltpu.roll(jnp.where(row == 7, ref[rows_of(block - 1), :], q), 1, 0)
        below = pltpu.roll(jnp.where(row == 0, ref[rows_of(block + 1), :], q), 7, 0)
        return q, above, below

    def kicked(q, above, below, beside, moment, share):
        near = (above + below) + beside
        return moment + (near * (share * a) - q * (q * q * (share * g) + share * b))

    def leap(src, src_at, mom, mom_at, dst, dst_p, at, first):
        q, above, below = around(src, src_at)
        beside, _ = lateral(q)
        moment = mom[rows_of(mom_at), :]
        moment = kicked(q, above, below, beside, moment, 0.5 if first else 1.0)
        dst_p[rows_of(at), :] = moment
        dst[rows_of(at), :] = q + EPS * moment

    def finish(src, src_at, mom, mom_at, start_at, sums):
        q, above, below = around(src, src_at)
        beside, right = lateral(q)
        moment = kicked(q, above, below, beside, mom[rows_of(mom_at), :], 0.5)
        new = site(q, below, right)
        p, _, p_below = around(q0, start_at)
        old = site(p, p_below, lateral(p)[1])
        start = m0[rows_of(start_at), :]
        change = (0.5 * moment * moment + coldness * new) - (0.5 * start * start + coldness * old)
        return sums[0] + fold(change), sums[1] + fold(jnp.where(accepted, new, old))

    def inner(src, dst, mom, first):
        def some(n, carry):
            for k in range(7):
                at = 3 + 7 * n + k
                leap(src, at, mom, at, dst, pa, at, first)
            return carry

        lax.fori_loop(0, 2, some, 0)

    def inner_pair(n, carry):
        inner(qa_0, qa_1, pa, False)
        inner(qa_1, qa_0, pa, False)
        return carry

    inner(q0, qa_0, m0, True)
    lax.fori_loop(0, 3, inner_pair, 0)
    inner(qa_0, qa_1, pa, False)
    zero = jnp.zeros((8, 128), F32)
    for part in range(2):
        first = 32 + 32 * part
        settle(joined(qa_1[pl.ds(16 + first, 32), :]), [(0, 32, first)])

    def to_column(src, tab, send_sem, recv_sem):
        for k in range(8):
            push(src, tab.at[place], send_sem, recv_sem, join_rep(x, (z + k) % 8, y, c))

    def to_plane(tab, dst, send_sem, recv_sem):
        block = pl.ds(pl.multiple_of(group * 8, 8), 8)
        for k in range(16):
            push(
                tab.at[block], dst.at[block], send_sem, recv_sem,
                join_rep((x + k // 4) % 4, z, (y + (k // 2) % 2) % 2, (c + k % 2) % 2),
            )

    def spread(chunk, first=0, last=128):
        def one(k, carry):
            home = lax.rem(me + k, 128)
            push(tile_of(out_ref, chunk, home), got[chunk].at[me], send_1.at[chunk], recv_1.at[chunk], home)
            return carry

        lax.fori_loop(first, last, one, 0, unroll=4)

    def pick(chunk):
        def one(t, carry):
            picked[chunk][t] = got[chunk][holder_ref[0, t]]
            return carry

        lax.fori_loop(0, 128, one, 0, unroll=8)

    def give(chunk):
        def one(k, carry):
            goal = lax.rem(me + k, 128)
            push(picked[chunk].at[goal], tile_of(sorted_ref, chunk, me), send_2.at[chunk], recv_2, goal)
            return carry

        lax.fori_loop(0, 128, one, 0, unroll=4)

    halos = ((q0, 136, 8), (q0, 16, 144), (m0, 136, 8), (m0, 16, 144))
    edges = ((q0, 135, 7), (q0, 24, 152))

    def halo(k, n):
        ref, src_row, dst_row = halos[k]
        cols = pl.ds(pl.multiple_of(256 * n, 128), 256)
        push(
            ref.at[pl.ds(src_row, 8), cols], ref.at[pl.ds(dst_row, 8), cols],
            send_h.at[k], recv_h.at[k], me,
        )

    pl.semaphore_wait(barrier, 128)
    to_column(label_row, label_tab.at[0], send_lab.at[0], recv_lab.at[0])
    for k, (ref, src_row, dst_row) in enumerate(edges):
        push(ref.at[pl.ds(src_row, 1)], ref.at[pl.ds(dst_row, 1)], send_h.at[4 + k], recv_h.at[4 + k], me)

    def spread_and_halo(n, carry):
        for k in range(4):
            halo(k, n)
            for at in range(4):
                home = lax.rem(me + 16 * n + 4 * k + at, 128)
                push(tile_of(out_ref, 0, home), got_0.at[me], send_1.at[0], recv_1.at[0], home)
        return carry

    lax.fori_loop(0, 4, spread_and_halo, 0)
    wait_for(label_tab.at[0, pl.ds(0, 8)], recv_lab.at[0])
    to_plane(label_tab.at[0], label_tab.at[1], send_lab.at[1], recv_lab.at[1])
    lax.fori_loop(4, 8, spread_and_halo, 0)
    settle(
        joined(jnp.concatenate((qa_1[pl.ds(32, 16), :], qa_1[pl.ds(112, 16), :]), 0)),
        [(0, 16, 16), (16, 16, 96)],
    )
    spread(1)

    def inner_last(i, sums):
        return finish(qa_1, i, pa, i, i, sums)

    sums = lax.fori_loop(4, 16, inner_last, (zero, zero))

    lane = lax.broadcasted_iota(jnp.int32, (1, 128), 1)
    wait_for(label_tab.at[1], recv_lab.at[1])
    holder = jnp.zeros((1, 128), jnp.int32)
    for p in range(128):
        rep = join_rep(p // 32, p % 8, (p // 16) % 2, (p // 8) % 2)
        holder = jnp.maximum(holder, jnp.where(label_tab[1, p] == lane, rep, 0))
    holder_row[...] = holder
    copy = pltpu.make_async_copy(holder_row, holder_ref, local_sem)
    copy.start()
    copy.wait()

    wait_for(got_0, recv_1.at[0])
    pick(0)
    give(0)

    for k, (ref, src_row, dst_row) in enumerate(halos):
        wait_for(ref.at[pl.ds(dst_row, 8)], recv_h.at[k])
    for k, (ref, src_row, dst_row) in enumerate(edges):
        wait_for(ref.at[pl.ds(dst_row, 1)], recv_h.at[4 + k])

    def outer(src, dst, mom, first):
        def some(side, carry):
            for k in range(1, 5):
                at = (14 if first else 6) * side + k
                leap(src, at, mom, at, dst, pe, 6 * side + k, first)
            return carry

        lax.fori_loop(0, 2, some, 0)

    def outer_pair(n, carry):
        outer(qe_0, qe_1, pe, False)
        outer(qe_1, qe_0, pe, False)
        return carry

    outer(q0, qe_0, m0, True)
    lax.fori_loop(0, 3, outer_pair, 0)
    outer(qe_0, qe_1, pe, False)
    settle(
        joined(jnp.concatenate((qe_1[pl.ds(16, 16), :], qe_1[pl.ds(64, 16), :]), 0)),
        [(0, 16, 0), (16, 16, 112)],
    )
    spread(2)
    stores.append(pltpu.make_async_copy(out_ref, out_hbm, store_sem.at[1]))
    stores[1].start()

    def outer_last(i, sums):
        side, local = lax.div(i, 2), 2 + lax.rem(i, 2)
        return finish(qe_1, 6 * side + local, pe, 6 * side + local, 14 * side + local, sums)

    sums = lax.fori_loop(0, 4, outer_last, sums)
    act_row[...] = jnp.where(lane == 0, jnp.sum(sums[1]), jnp.where(lane == 1, jnp.sum(sums[0]), 0.0))
    push(act_row, act_got, send_act.at[0], recv_act.at[0], me)

    wait_for(got_1, recv_1.at[1])
    pick(1)
    give(1)
    wait_for(act_got, recv_act.at[0])
    total = act_row[...] + act_got[...]
    act_sum[...] = total
    to_column(act_sum, act_tab.at[0], send_act.at[1], recv_act.at[1])
    wait_for(got_2, recv_1.at[2])
    pick(2)
    wait_for(act_tab.at[0, pl.ds(0, 8)], recv_act.at[1])
    to_plane(act_tab.at[0], act_tab.at[1], send_act.at[2], recv_act.at[2])
    give(2)

    for k, (ref, src_row, dst_row) in enumerate(halos):
        wait_for(ref.at[pl.ds(src_row, 8)], send_h.at[k])
    for k, (ref, src_row, dst_row) in enumerate(edges):
        wait_for(ref.at[pl.ds(src_row, 1)], send_h.at[4 + k])
    wait_for(label_tab.at[0, pl.ds(0, 8)], send_lab.at[0])
    wait_for(label_tab.at[1], send_lab.at[1])
    wait_for(act_got, send_act.at[0])
    wait_for(act_tab.at[0, pl.ds(0, 8)], send_act.at[1])
    for chunk in range(3):
        wait_for(got[chunk], send_1.at[chunk])
    change_ref[0] = jnp.sum(jnp.where(lane == 1, total, 0.0))
    stores.append(pltpu.make_async_copy(change_ref, change_hbm, store_sem.at[2]))
    stores[2].start()
    wait_for(act_tab.at[1], recv_act.at[2])
    ladder = jnp.zeros((1, 128), F32)
    for p in range(128):
        ladder = ladder + jnp.where(label_tab[1, p] == me, act_tab[1, p], 0.0)
    ladder_ref[0] = jnp.sum(jnp.where(lane == 0, ladder, 0.0)) / 524288.0
    stores.append(pltpu.make_async_copy(ladder_ref, ladder_hbm, store_sem.at[3]))
    stores[3].start()
    for copy in stores:
        copy.wait()
    wait_for(act_tab.at[1], send_act.at[2])
    for chunk in range(3):
        wait_for(got[chunk], send_2.at[chunk])
    wait_for(sorted_ref, recv_2)


def hand_over(*refs):
    given, results, held, load_sem, store_sem, small_sem = refs[:5], refs[5:10], refs[10], refs[11], refs[12], refs[13]
    small = [pltpu.make_async_copy(given[k], results[k], small_sem.at[k - 2]) for k in range(2, 5)]
    for copy in small:
        copy.start()
    loads, stores = [], []
    for k in range(2):
        for n in range(4):
            part = pl.ds(4 * n, 4)
            loads.append(pltpu.make_async_copy(given[k].at[part], held.at[k, part], load_sem.at[4 * k + n]))
            stores.append(pltpu.make_async_copy(held.at[k, part], results[k].at[part], store_sem.at[4 * k + n]))
    for copy in loads:
        copy.start()
    for load, store in zip(loads, stores):
        load.wait()
        store.start()
    for copy in stores + small:
        copy.wait()


def body(field, momentum, labels, betas, accept, swap_pairs):
    i32 = jnp.int32
    dma = pltpu.SemaphoreType.DMA
    strip = jax.ShapeDtypeStruct((16, 8, 2048), F32)
    hbm = pl.BlockSpec(memory_space=pltpu.HBM)
    shapes = (
        strip, strip, jax.ShapeDtypeStruct((1,), i32),
        jax.ShapeDtypeStruct((1,), F32), jax.ShapeDtypeStruct((1,), F32),
    )
    results = pl.pallas_call(
        whole,
        out_shape=shapes,
        in_specs=[hbm] * 6,
        out_specs=(hbm,) * 5,
        scratch_shapes=[
            pltpu.SMEM((1,), i32),
            pltpu.SMEM((128,), F32),
            pltpu.SMEM((1,), i32),
            pltpu.SMEM((128,), i32),
            pltpu.SMEM((1,), i32),
            pltpu.SMEM((1,), F32),
            pltpu.SMEM((1,), F32),
            pltpu.VMEM((16, 8, 2048), F32),
            pltpu.VMEM((128, 2048), F32),
            pltpu.VMEM((128, 2048), F32),
            pltpu.VMEM((160, 2048), F32),
            pltpu.VMEM((160, 2048), F32),
            pltpu.VMEM((160, 2048), F32),
            pltpu.VMEM((160, 2048), F32),
            pltpu.VMEM((160, 2048), F32),
            pltpu.VMEM((96, 2048), F32),
            pltpu.VMEM((96, 2048), F32),
            pltpu.VMEM((96, 2048), F32),
            pltpu.VMEM((768, 256), BF16),
            pltpu.VMEM((512, 256), BF16),
            pltpu.VMEM((128, 8, 128), F32),
            pltpu.VMEM((128, 4, 128), F32),
            pltpu.VMEM((128, 4, 128), F32),
            pltpu.VMEM((128, 8, 128), F32),
            pltpu.VMEM((128, 4, 128), F32),
            pltpu.VMEM((128, 4, 128), F32),
            pltpu.VMEM((1, 128), i32),
            pltpu.VMEM((2, 128, 1, 128), i32),
            pltpu.VMEM((1, 128), F32),
            pltpu.VMEM((1, 128), F32),
            pltpu.VMEM((1, 128), F32),
            pltpu.VMEM((2, 128, 1, 128), F32),
            pltpu.VMEM((1, 128), i32),
            pltpu.SMEM((1, 128), i32),
            dma((6,)), dma((6,)), dma((3,)), dma((3,)), dma((3,)), dma(()),
            dma((2,)), dma((2,)), dma((3,)), dma((3,)), dma(()), dma((2,)), dma((4,)), dma((4,)),
        ],
        compiler_params=pltpu.CompilerParams(collective_id=0, has_side_effects=True, vmem_limit_bytes=67_000_000),
    )(field, momentum, labels, betas, accept, swap_pairs)
    out, ordered, new_label, change, ladder = pl.pallas_call(
        hand_over,
        out_shape=shapes,
        in_specs=[hbm] * 5,
        out_specs=(hbm,) * 5,
        scratch_shapes=[pltpu.VMEM((2, 16, 8, 2048), F32), dma((8,)), dma((8,)), dma((3,))],
        compiler_params=pltpu.CompilerParams(vmem_limit_bytes=67_000_000),
    )(*results)
    return out.reshape(1, 128, 2048), ordered.reshape(1, 128, 2048), new_label, change, ladder


def solution(mesh):
    rep = P("rep")
    strip = P("rep", "dom", None)
    in_specs = (strip, strip, rep, P(), rep, P())
    out_specs = (strip, strip, rep, rep, rep)
    return jax.shard_map(body, mesh=mesh, in_specs=in_specs, out_specs=out_specs, check_vma=False)
```

```python
import functools
import jax
import jax.numpy as jnp
from jax import lax
from jax.experimental import pallas as pl
from jax.experimental.pallas import tpu as pltpu
from jax.sharding import PartitionSpec as P

MESH = pl.DeviceIdType.MESH

HOP = 0.36
QUARTIC = 0.3
EPS = 0.05
F32 = jnp.float32
BF16 = jnp.bfloat16

def split_rep(rep):
    return rep // 32, (rep // 4) % 8, (rep // 2) % 2, rep % 2


def join_rep(x, z, y, c):
    return ((x * 8 + z) * 2 + y) * 2 + c


def table_place(rep):
    x, z, y, c = split_rep(rep)
    return ((x * 2 + y) * 2 + c) * 8 + z


def tile_of(ref, chunk, home):
    cols = pl.ds(pl.multiple_of(lax.rem(home, 16) * 128, 128), 128)
    if chunk == 1:
        b = lax.div(home, 16)
        return ref.at[2 + b + 4 * lax.div(b, 4), :, cols]
    b = lax.div(home, 32)
    block = 6 + b if chunk == 0 else b + 12 * lax.div(b, 2)
    half = pl.ds(pl.multiple_of(4 * lax.rem(lax.div(home, 16), 2), 4), 4)
    return ref.at[block, half, cols]


def wait_for(ref, sem):
    pltpu.make_async_copy(ref, ref, sem).wait()


def rows_of(block):
    return pl.ds(pl.multiple_of(block * 8, 8), 8)


def lateral(q):
    even, odd = q[:, :1024], q[:, 1024:]
    after = pltpu.roll(even, 1023, 1)
    return jnp.concatenate((odd + pltpu.roll(odd, 1, 1), even + after), 1), jnp.concatenate((odd, after), 1)


def fold(v):
    total = v[:, :128]
    for j in range(1, 16):
        total = total + v[:, 128 * j : 128 * j + 128]
    return total


def split_two(v):
    high = v.astype(BF16)
    return high, (v - high.astype(F32)).astype(BF16)


def site(q, below, right):
    squared = q * q
    return -HOP * q * (below + right) + squared + QUARTIC * (squared - 1.0) * (squared - 1.0)


def whole(
    field_hbm, moment_hbm, labels_hbm, betas_hbm, accept_hbm, pairs_hbm,
    out_ref, sorted_ref, new_hbm, change_hbm, ladder_hbm,
    labels_ref, betas_ref, accept_ref, pairs_ref, new_ref, change_ref, ladder_ref,
    field_ref, moment_ref, q0, m0, qa_0, qa_1, pa, qe_0, qe_1, pe, perm, perm_back,
    got_0, got_1, got_2, picked_0, picked_1, picked_2, label_row, label_tab, act_row, act_got, act_sum, act_tab, holder_row, holder_ref,
    send_h, recv_h, send_1, recv_1, send_2, recv_2, send_lab, recv_lab, send_act, recv_act, local_sem, load_sem, small_sem, store_sem,
):
    me = lax.axis_index("rep")
    dom = lax.axis_index("dom")
    other = 1 - dom
    x, z, y, c = split_rep(me)
    place = table_place(me)
    group = lax.div(place, 8)
    got = (got_0, got_1, got_2)
    picked = (picked_0, picked_1, picked_2)

    loads = []
    for first, n in ((32, 64), (0, 32), (96, 32)):
        rows = pl.ds(first, n)
        for src, dst in ((field_hbm, field_ref), (moment_hbm, moment_ref)):
            loads.append(pltpu.make_async_copy(src.at[0, rows], dst.at[rows], load_sem.at[len(loads)]))
            loads[-1].start()
    small = []
    for k, (src, dst) in enumerate(
        ((labels_hbm, labels_ref), (betas_hbm, betas_ref), (accept_hbm, accept_ref), (pairs_hbm, pairs_ref))
    ):
        small.append(pltpu.make_async_copy(src, dst, small_sem.at[k]))
        small[k].start()

    def push(src, dst, send_sem, recv_sem, rep):
        pltpu.make_async_remote_copy(
            src_ref=src, dst_ref=dst, send_sem=send_sem, recv_sem=recv_sem,
            device_id=(rep, other), device_id_type=MESH,
        ).start()

    barrier = pltpu.get_barrier_semaphore()

    xs = [lax.rem(x + k, 4) * 32 for k in (2, 1, 3, 0)]
    zs = [lax.rem(z + k, 8) * 4 for k in (4, 3, 5, 2, 6, 1, 7, 0)]
    for at_z in zs:
        for at_x in xs:
            for k in range(4):
                pl.semaphore_signal(barrier, inc=1, device_id=(at_x + at_z + k, other), device_id_type=MESH)

    for copy in small:
        copy.wait()
    label = labels_ref[0]
    coldness = betas_ref[label]
    new_label = pairs_ref[label]
    accepted = accept_ref[0] == 1
    new_ref[0] = new_label
    stores = [pltpu.make_async_copy(new_ref, new_hbm, store_sem.at[0])]
    stores[0].start()
    label_row[...] = jnp.full((1, 128), new_label, jnp.int32)

    i0 = lax.broadcasted_iota(jnp.int32, (256, 256), 0)
    i1 = lax.broadcasted_iota(jnp.int32, (256, 256), 1)
    there = jnp.where(i1 < 128, 2 * i1, 2 * i1 - 255) == i0
    back = jnp.where(i0 < 128, 2 * i0, 2 * i0 - 255) == i1
    for third in range(3):
        perm[pl.ds(256 * third, 256), :] = jnp.where(there, 1.0, 0.0).astype(BF16)
    for half in range(2):
        perm_back[pl.ds(256 * half, 256), :] = jnp.where(back, 1.0, 0.0).astype(BF16)

    def apart(ref, dst, r):
        values = ref[pl.ds(pl.multiple_of(32 * r, 32), 32), :]
        high = values.astype(BF16)
        pieces = (high, *split_two(values - high.astype(F32)))
        cols = [slice(256 * b, 256 * b + 256) for b in range(8)]
        left = jnp.concatenate([jnp.concatenate([v[:, s] for v in pieces], 1) for s in cols], 0)
        res = jnp.dot(left, perm[...], preferred_element_type=F32)
        rows = pl.ds(pl.multiple_of(16 + 32 * r, 16), 32)
        for b in range(8):
            dst[rows, 128 * b : 128 * b + 128] = res[32 * b : 32 * b + 32, :128]
            dst[rows, 1024 + 128 * b : 1152 + 128 * b] = res[32 * b : 32 * b + 32, 128:]

    def joined(values):
        high, low = split_two(values)
        parts = []
        for b in range(8):
            e = slice(128 * b, 128 * b + 128)
            o = slice(1024 + 128 * b, 1152 + 128 * b)
            parts.append(jnp.concatenate((high[:, e], high[:, o], low[:, e], low[:, o]), 1))
        res = jnp.dot(jnp.concatenate(parts, 0), perm_back[...], preferred_element_type=F32)
        return jnp.concatenate([res[32 * b : 32 * b + 32] for b in range(8)], 1)

    def settle(values, rows):
        for at, n, first in rows:
            new = jnp.where(accepted, values[at : at + n], field_ref[pl.ds(first, n), :])
            out_ref[pl.ds(first // 8, n // 8)] = new.reshape(n // 8, 8, 2048)

    def set_apart(first, stride):
        def one(n, carry):
            apart(field_ref, q0, first + stride * n)
            apart(moment_ref, m0, first + stride * n)
            return carry

        lax.fori_loop(0, 2, one, 0)

    loads[0].wait()
    loads[1].wait()
    set_apart(1, 1)

    row = lax.broadcasted_iota(jnp.int32, (8, 2048), 0)
    a = coldness * (EPS * HOP)
    b = coldness * (EPS * (2.0 - 4.0 * QUARTIC))
    g = coldness * (EPS * 4.0 * QUARTIC)

    def around(ref, block):
        q = ref[rows_of(block), :]
        above = pltpu.roll(jnp.where(row == 7, ref[rows_of(block - 1), :], q), 1, 0)
        below = pltpu.roll(jnp.where(row == 0, ref[rows_of(block + 1), :], q), 7, 0)
        return q, above, below

    def kicked(q, above, below, beside, moment, share):
        near = (above + below) + beside
        return moment + (near * (share * a) - q * (q * q * (share * g) + share * b))

    def leap(src, src_at, mom, mom_at, dst, dst_p, at, first):
        q, above, below = around(src, src_at)
        beside, _ = lateral(q)
        moment = mom[rows_of(mom_at), :]
        moment = kicked(q, above, below, beside, moment, 0.5 if first else 1.0)
        dst_p[rows_of(at), :] = moment
        dst[rows_of(at), :] = q + EPS * moment

    def finish(src, src_at, mom, mom_at, start_at, sums):
        q, above, below = around(src, src_at)
        beside, right = lateral(q)
        moment = kicked(q, above, below, beside, mom[rows_of(mom_at), :], 0.5)
        new = site(q, below, right)
        p, _, p_below = around(q0, start_at)
        old = site(p, p_below, lateral(p)[1])
        start = m0[rows_of(start_at), :]
        change = (0.5 * moment * moment + coldness * new) - (0.5 * start * start + coldness * old)
        return sums[0] + fold(change), sums[1] + fold(jnp.where(accepted, new, old))

    def inner(base, count):
        def sweep(src, dst, mom, first):
            def some(n, carry):
                for k in range(6):
                    at = base + 8 * n + k
                    leap(src, at, mom, at, dst, pa, at, first)
                return carry

            lax.fori_loop(0, count, some, 0)

        def pair(n, carry):
            sweep(qa_0, qa_1, pa, False)
            sweep(qa_1, qa_0, pa, False)
            return carry

        sweep(q0, qa_0, m0, True)
        lax.fori_loop(0, 3, pair, 0)
        sweep(qa_0, qa_1, pa, False)

    def inner_last(first, last, sums):
        return lax.fori_loop(first, last, lambda i, sums: finish(qa_1, i, pa, i, i, sums), sums)

    inner(7, 1)
    settle(joined(qa_1[pl.ds(64, 32), :]), [(0, 32, 48)])

    def to_column(src, tab, send_sem, recv_sem):
        for k in range(8):
            push(src, tab.at[place], send_sem, recv_sem, join_rep(x, (z + k) % 8, y, c))

    def to_plane(tab, dst, send_sem, recv_sem):
        block = pl.ds(pl.multiple_of(group * 8, 8), 8)
        for k in range(16):
            push(
                tab.at[block], dst.at[block], send_sem, recv_sem,
                join_rep((x + k // 4) % 4, z, (y + (k // 2) % 2) % 2, (c + k % 2) % 2),
            )

    def spread(chunk, first=0, last=128):
        def one(k, carry):
            home = lax.rem(me + k, 128)
            push(tile_of(out_ref, chunk, home), got[chunk].at[me], send_1.at[chunk], recv_1.at[chunk], home)
            return carry

        lax.fori_loop(first, last, one, 0, unroll=4)

    def pick(chunk):
        def one(t, carry):
            picked[chunk][t] = got[chunk][holder_ref[0, t]]
            return carry

        lax.fori_loop(0, 128, one, 0, unroll=8)

    def give(chunk):
        def one(k, carry):
            goal = lax.rem(me + k, 128)
            push(picked[chunk].at[goal], tile_of(sorted_ref, chunk, me), send_2.at[chunk], recv_2, goal)
            return carry

        lax.fori_loop(0, 128, one, 0, unroll=4)

    halos = ((q0, 136, 8), (q0, 16, 144), (m0, 136, 8), (m0, 16, 144))
    edges = ((q0, 135, 7), (q0, 24, 152))

    def halo(k, n):
        ref, src_row, dst_row = halos[k]
        cols = pl.ds(pl.multiple_of(256 * n, 128), 256)
        push(
            ref.at[pl.ds(src_row, 8), cols], ref.at[pl.ds(dst_row, 8), cols],
            send_h.at[k], recv_h.at[k], me,
        )

    pl.semaphore_wait(barrier, 128)
    to_column(label_row, label_tab.at[0], send_lab.at[0], recv_lab.at[0])
    spread(0)
    zero = jnp.zeros((8, 128), F32)
    sums = inner_last(8, 12, (zero, zero))
    for load in loads[2:]:
        load.wait()
    set_apart(0, 3)
    wait_for(label_tab.at[0, pl.ds(0, 8)], recv_lab.at[0])
    to_plane(label_tab.at[0], label_tab.at[1], send_lab.at[1], recv_lab.at[1])
    inner(3, 2)
    for part in range(2):
        settle(joined(qa_1[pl.ds(32 + 64 * part, 32), :]), [(0, 32, 16 + 64 * part)])

    for k, (ref, src_row, dst_row) in enumerate(edges):
        push(ref.at[pl.ds(src_row, 1)], ref.at[pl.ds(dst_row, 1)], send_h.at[4 + k], recv_h.at[4 + k], me)

    def spread_and_halo(n, carry):
        for k in range(4):
            halo(k, n)
            for at in range(4):
                home = lax.rem(me + 16 * n + 4 * k + at, 128)
                push(tile_of(out_ref, 1, home), got_1.at[me], send_1.at[1], recv_1.at[1], home)
        return carry

    lax.fori_loop(0, 8, spread_and_halo, 0)

    lane = lax.broadcasted_iota(jnp.int32, (1, 128), 1)
    wait_for(label_tab.at[1], recv_lab.at[1])
    holder = jnp.zeros((1, 128), jnp.int32)
    for p in range(128):
        rep = join_rep(p // 32, p % 8, (p // 16) % 2, (p // 8) % 2)
        holder = jnp.maximum(holder, jnp.where(label_tab[1, p] == lane, rep, 0))
    holder_row[...] = holder
    copy = pltpu.make_async_copy(holder_row, holder_ref, local_sem)
    copy.start()
    copy.wait()

    wait_for(got_0, recv_1.at[0])
    pick(0)
    give(0)
    sums = inner_last(4, 8, sums)
    sums = inner_last(12, 16, sums)

    for k, (ref, src_row, dst_row) in enumerate(halos):
        wait_for(ref.at[pl.ds(dst_row, 8)], recv_h.at[k])
    for k, (ref, src_row, dst_row) in enumerate(edges):
        wait_for(ref.at[pl.ds(dst_row, 1)], recv_h.at[4 + k])

    def outer(src, dst, mom, first):
        def some(side, carry):
            for k in range(1, 5):
                at = (14 if first else 6) * side + k
                leap(src, at, mom, at, dst, pe, 6 * side + k, first)
            return carry

        lax.fori_loop(0, 2, some, 0)

    def outer_pair(n, carry):
        outer(qe_0, qe_1, pe, False)
        outer(qe_1, qe_0, pe, False)
        return carry

    outer(q0, qe_0, m0, True)
    lax.fori_loop(0, 3, outer_pair, 0)
    outer(qe_0, qe_1, pe, False)
    settle(
        joined(jnp.concatenate((qe_1[pl.ds(16, 16), :], qe_1[pl.ds(64, 16), :]), 0)),
        [(0, 16, 0), (16, 16, 112)],
    )
    spread(2)

    def outer_last(i, sums):
        side, local = lax.div(i, 2), 2 + lax.rem(i, 2)
        return finish(qe_1, 6 * side + local, pe, 6 * side + local, 14 * side + local, sums)

    sums = lax.fori_loop(0, 4, outer_last, sums)
    act_row[...] = jnp.where(lane == 0, jnp.sum(sums[1]), jnp.where(lane == 1, jnp.sum(sums[0]), 0.0))
    push(act_row, act_got, send_act.at[0], recv_act.at[0], me)

    wait_for(got_1, recv_1.at[1])
    pick(1)
    give(1)
    wait_for(act_got, recv_act.at[0])
    total = act_row[...] + act_got[...]
    act_sum[...] = total
    to_column(act_sum, act_tab.at[0], send_act.at[1], recv_act.at[1])
    wait_for(got_2, recv_1.at[2])
    pick(2)
    wait_for(act_tab.at[0, pl.ds(0, 8)], recv_act.at[1])
    to_plane(act_tab.at[0], act_tab.at[1], send_act.at[2], recv_act.at[2])
    give(2)

    for k, (ref, src_row, dst_row) in enumerate(halos):
        wait_for(ref.at[pl.ds(src_row, 8)], send_h.at[k])
    for k, (ref, src_row, dst_row) in enumerate(edges):
        wait_for(ref.at[pl.ds(src_row, 1)], send_h.at[4 + k])
    wait_for(label_tab.at[0, pl.ds(0, 8)], send_lab.at[0])
    wait_for(label_tab.at[1], send_lab.at[1])
    wait_for(act_got, send_act.at[0])
    wait_for(act_tab.at[0, pl.ds(0, 8)], send_act.at[1])
    for chunk in range(3):
        wait_for(got[chunk], send_1.at[chunk])
    change_ref[0] = jnp.sum(jnp.where(lane == 1, total, 0.0))
    stores.append(pltpu.make_async_copy(change_ref, change_hbm, store_sem.at[1]))
    stores[1].start()
    wait_for(act_tab.at[1], recv_act.at[2])
    ladder = jnp.zeros((1, 128), F32)
    for p in range(128):
        ladder = ladder + jnp.where(label_tab[1, p] == me, act_tab[1, p], 0.0)
    ladder_ref[0] = jnp.sum(jnp.where(lane == 0, ladder, 0.0)) / 524288.0
    stores.append(pltpu.make_async_copy(ladder_ref, ladder_hbm, store_sem.at[2]))
    stores[2].start()
    for copy in stores:
        copy.wait()
    wait_for(act_tab.at[1], send_act.at[2])
    for chunk in range(3):
        wait_for(got[chunk], send_2.at[chunk])
    wait_for(sorted_ref, recv_2)


def hand_over(out_in, sorted_in, new_in, change_in, ladder_in, out, ordered, new, change, ladder, sems):
    pairs = ((out_in, out), (sorted_in, ordered), (new_in, new), (change_in, change), (ladder_in, ladder))
    copies = [pltpu.make_async_copy(src, dst, sems.at[k]) for k, (src, dst) in enumerate(pairs)]
    for copy in copies:
        copy.start()
    for copy in copies:
        copy.wait()


def body(field, momentum, labels, betas, accept, swap_pairs):
    i32 = jnp.int32
    dma = pltpu.SemaphoreType.DMA
    strip = jax.ShapeDtypeStruct((16, 8, 2048), F32)
    hbm = pl.BlockSpec(memory_space=pltpu.HBM)
    vmem = pl.BlockSpec(memory_space=pltpu.VMEM)
    shapes = (
        strip, strip, jax.ShapeDtypeStruct((1,), i32),
        jax.ShapeDtypeStruct((1,), F32), jax.ShapeDtypeStruct((1,), F32),
    )
    results = pl.pallas_call(
        whole,
        out_shape=shapes,
        in_specs=[hbm] * 6,
        out_specs=(vmem, vmem, hbm, hbm, hbm),
        scratch_shapes=[
            pltpu.SMEM((1,), i32),
            pltpu.SMEM((128,), F32),
            pltpu.SMEM((1,), i32),
            pltpu.SMEM((128,), i32),
            pltpu.SMEM((1,), i32),
            pltpu.SMEM((1,), F32),
            pltpu.SMEM((1,), F32),
            pltpu.VMEM((128, 2048), F32),
            pltpu.VMEM((128, 2048), F32),
            pltpu.VMEM((160, 2048), F32),
            pltpu.VMEM((160, 2048), F32),
            pltpu.VMEM((160, 2048), F32),
            pltpu.VMEM((160, 2048), F32),
            pltpu.VMEM((160, 2048), F32),
            pltpu.VMEM((96, 2048), F32),
            pltpu.VMEM((96, 2048), F32),
            pltpu.VMEM((96, 2048), F32),
            pltpu.VMEM((768, 256), BF16),
            pltpu.VMEM((512, 256), BF16),
            pltpu.VMEM((128, 4, 128), F32),
            pltpu.VMEM((128, 8, 128), F32),
            pltpu.VMEM((128, 4, 128), F32),
            pltpu.VMEM((128, 4, 128), F32),
            pltpu.VMEM((128, 8, 128), F32),
            pltpu.VMEM((128, 4, 128), F32),
            pltpu.VMEM((1, 128), i32),
            pltpu.VMEM((2, 128, 1, 128), i32),
            pltpu.VMEM((1, 128), F32),
            pltpu.VMEM((1, 128), F32),
            pltpu.VMEM((1, 128), F32),
            pltpu.VMEM((2, 128, 1, 128), F32),
            pltpu.VMEM((1, 128), i32),
            pltpu.SMEM((1, 128), i32),
            dma((6,)), dma((6,)), dma((3,)), dma((3,)), dma((3,)), dma(()),
            dma((2,)), dma((2,)), dma((3,)), dma((3,)), dma(()), dma((6,)), dma((4,)), dma((3,)),
        ],
        compiler_params=pltpu.CompilerParams(collective_id=0, has_side_effects=True, vmem_limit_bytes=53_500_000),
    )(field, momentum, labels, betas, accept, swap_pairs)
    out, ordered, new_label, change, ladder = pl.pallas_call(
        hand_over,
        out_shape=shapes,
        in_specs=[vmem, vmem, hbm, hbm, hbm],
        out_specs=(hbm,) * 5,
        scratch_shapes=[dma((5,))],
        compiler_params=pltpu.CompilerParams(vmem_limit_bytes=8 << 20),
    )(*results)
    return out.reshape(1, 128, 2048), ordered.reshape(1, 128, 2048), new_label, change, ladder


def solution(mesh):
    rep = P("rep")
    strip = P("rep", "dom", None)
    in_specs = (strip, strip, rep, P(), rep, P())
    out_specs = (strip, strip, rep, rep, rep)
    return jax.shard_map(body, mesh=mesh, in_specs=in_specs, out_specs=out_specs, check_vma=False)
```

```python
import functools
import jax
import jax.numpy as jnp
from jax import lax
from jax.experimental import pallas as pl
from jax.experimental.pallas import tpu as pltpu
from jax.sharding import PartitionSpec as P

MESH = pl.DeviceIdType.MESH

HOP = 0.36
QUARTIC = 0.3
EPS = 0.05
F32 = jnp.float32
BF16 = jnp.bfloat16

def split_rep(rep):
    return rep // 32, (rep // 4) % 8, (rep // 2) % 2, rep % 2


def join_rep(x, z, y, c):
    return ((x * 8 + z) * 2 + y) * 2 + c


def table_place(rep):
    x, z, y, c = split_rep(rep)
    return ((x * 2 + y) * 2 + c) * 8 + z


def half_tile(ref, chunk, part, at):
    b, half = lax.div(part, 2), pl.ds(pl.multiple_of(4 * lax.rem(part, 2), 4), 4)
    block = b + 12 * lax.div(b, 2) if chunk == 3 else (6, 2, 10)[chunk] + b
    return ref.at[block, half, pl.ds(pl.multiple_of(128 * at, 128), 128)]


def wait_for(ref, sem):
    pltpu.make_async_copy(ref, ref, sem).wait()


def rows_of(block):
    return pl.ds(pl.multiple_of(block * 8, 8), 8)


def lateral(q):
    even, odd = q[:, :1024], q[:, 1024:]
    after = pltpu.roll(even, 1023, 1)
    return jnp.concatenate((odd + pltpu.roll(odd, 1, 1), even + after), 1), jnp.concatenate((odd, after), 1)


def fold(v):
    total = v[:, :128]
    for j in range(1, 16):
        total = total + v[:, 128 * j : 128 * j + 128]
    return total


def split_two(v):
    high = v.astype(BF16)
    return high, (v - high.astype(F32)).astype(BF16)


def site(q, below, right):
    squared = q * q
    return -HOP * q * (below + right) + squared + QUARTIC * (squared - 1.0) * (squared - 1.0)


CHUNKS = 4


def whole(
    field_hbm, moment_hbm, labels_hbm, betas_hbm, accept_hbm, pairs_hbm,
    out_ref, sorted_ref, label_out, act_out,
    labels_ref, betas_ref, accept_ref, pairs_ref,
    field_ref, moment_ref, q0, m0, qm_0, qm_1, pm, qa_0, qa_1, pa, qe_0, qe_1, pe, perm, perm_back,
    got_0, got_1, got_2, got_3, picked_0, picked_1, picked_2, picked_3, label_row, label_tab, act_row, act_got, act_sum, act_tab, holder_row, holder_ref,
    send_h, recv_h, send_1, recv_1, send_2, recv_2, send_lab, recv_lab, send_act, recv_act, local_sem, load_sem, small_sem,
):
    me = lax.axis_index("rep")
    dom = lax.axis_index("dom")
    other = 1 - dom
    x, z, y, c = split_rep(me)
    place = table_place(me)
    group = lax.div(place, 8)
    got = (got_0, got_1, got_2, got_3)
    picked = (picked_0, picked_1, picked_2, picked_3)
    part_of_me, lane_of_me = lax.div(me, 16), lax.rem(me, 16)
    turned = [lax.rem(lane_of_me + k, 16) for k in range(16)]

    loads = []
    for first, n in ((32, 64), (0, 32), (96, 32)):
        rows = pl.ds(first, n)
        for src, dst in ((field_hbm, field_ref), (moment_hbm, moment_ref)):
            loads.append(pltpu.make_async_copy(src.at[0, rows], dst.at[rows], load_sem.at[len(loads)]))
            loads[-1].start()
    small = []
    for k, (src, dst) in enumerate(
        ((labels_hbm, labels_ref), (betas_hbm, betas_ref), (accept_hbm, accept_ref), (pairs_hbm, pairs_ref))
    ):
        small.append(pltpu.make_async_copy(src, dst, small_sem.at[k]))
        small[k].start()

    def push(src, dst, send_sem, recv_sem, rep):
        pltpu.make_async_remote_copy(
            src_ref=src, dst_ref=dst, send_sem=send_sem, recv_sem=recv_sem,
            device_id=(rep, other), device_id_type=MESH,
        ).start()

    barrier = pltpu.get_barrier_semaphore()

    xs = [lax.rem(x + k, 4) * 32 for k in (2, 1, 3, 0)]
    zs = [lax.rem(z + k, 8) * 4 for k in (4, 3, 5, 2, 6, 1, 7, 0)]
    for at_z in zs:
        for at_x in xs:
            for k in range(4):
                pl.semaphore_signal(barrier, inc=1, device_id=(at_x + at_z + k, other), device_id_type=MESH)

    for copy in small:
        copy.wait()
    label = labels_ref[0]
    coldness = betas_ref[label]
    new_label = pairs_ref[label]
    accepted = accept_ref[0] == 1
    label_out[...] = jnp.full((1, 128), new_label, jnp.int32)
    label_row[...] = jnp.full((1, 128), new_label, jnp.int32)

    i0 = lax.broadcasted_iota(jnp.int32, (256, 256), 0)
    i1 = lax.broadcasted_iota(jnp.int32, (256, 256), 1)
    there = jnp.where(i1 < 128, 2 * i1, 2 * i1 - 255) == i0
    back = jnp.where(i0 < 128, 2 * i0, 2 * i0 - 255) == i1
    for third in range(3):
        perm[pl.ds(256 * third, 256), :] = jnp.where(there, 1.0, 0.0).astype(BF16)
    for half in range(2):
        perm_back[pl.ds(256 * half, 256), :] = jnp.where(back, 1.0, 0.0).astype(BF16)

    def apart(ref, dst, r):
        values = ref[pl.ds(pl.multiple_of(32 * r, 32), 32), :]
        high = values.astype(BF16)
        pieces = (high, *split_two(values - high.astype(F32)))
        cols = [slice(256 * b, 256 * b + 256) for b in range(8)]
        left = jnp.concatenate([jnp.concatenate([v[:, s] for v in pieces], 1) for s in cols], 0)
        res = jnp.dot(left, perm[...], preferred_element_type=F32)
        rows = pl.ds(pl.multiple_of(16 + 32 * r, 16), 32)
        for b in range(8):
            dst[rows, 128 * b : 128 * b + 128] = res[32 * b : 32 * b + 32, :128]
            dst[rows, 1024 + 128 * b : 1152 + 128 * b] = res[32 * b : 32 * b + 32, 128:]

    def joined(values):
        high, low = split_two(values)
        parts = []
        for b in range(8):
            e = slice(128 * b, 128 * b + 128)
            o = slice(1024 + 128 * b, 1152 + 128 * b)
            parts.append(jnp.concatenate((high[:, e], high[:, o], low[:, e], low[:, o]), 1))
        res = jnp.dot(jnp.concatenate(parts, 0), perm_back[...], preferred_element_type=F32)
        return jnp.concatenate([res[32 * b : 32 * b + 32] for b in range(8)], 1)

    def settle(values, rows):
        for at, n, first in rows:
            new = jnp.where(accepted, values[at : at + n], field_ref[pl.ds(first, n), :])
            out_ref[pl.ds(first // 8, n // 8)] = new.reshape(n // 8, 8, 2048)

    def set_apart(first, count):
        def one(n, carry):
            apart(field_ref, q0, first + n)
            apart(moment_ref, m0, first + n)
            return carry

        lax.fori_loop(0, count, one, 0)

    loads[0].wait()
    loads[1].wait()
    set_apart(1, 2)

    row = lax.broadcasted_iota(jnp.int32, (8, 2048), 0)
    a = coldness * (EPS * HOP)
    b = coldness * (EPS * (2.0 - 4.0 * QUARTIC))
    g = coldness * (EPS * 4.0 * QUARTIC)

    def around(ref, block):
        q = ref[rows_of(block), :]
        above = pltpu.roll(jnp.where(row == 7, ref[rows_of(block - 1), :], q), 1, 0)
        below = pltpu.roll(jnp.where(row == 0, ref[rows_of(block + 1), :], q), 7, 0)
        return q, above, below

    def kicked(q, above, below, beside, moment, share):
        near = (above + below) + beside
        return moment + (near * (share * a) - q * (q * q * (share * g) + share * b))

    def leap(src, src_at, mom, mom_at, dst, dst_p, at, first):
        q, above, below = around(src, src_at)
        beside, _ = lateral(q)
        moment = mom[rows_of(mom_at), :]
        moment = kicked(q, above, below, beside, moment, 0.5 if first else 1.0)
        dst_p[rows_of(at), :] = moment
        dst[rows_of(at), :] = q + EPS * moment

    def finish(src, src_at, mom, mom_at, start_at, sums):
        q, above, below = around(src, src_at)
        beside, right = lateral(q)
        moment = kicked(q, above, below, beside, mom[rows_of(mom_at), :], 0.5)
        new = site(q, below, right)
        p, _, p_below = around(q0, start_at)
        old = site(p, p_below, lateral(p)[1])
        start = m0[rows_of(start_at), :]
        change = (0.5 * moment * moment + coldness * new) - (0.5 * start * start + coldness * old)
        return sums[0] + fold(change), sums[1] + fold(jnp.where(accepted, new, old))

    def inner(even, odd, mom, base):
        def sweep(src, dst, src_p, first):
            for at in range(base, base + 6):
                leap(src, at, src_p, at, dst, mom, at, first)

        def pair(n, carry):
            sweep(even, odd, mom, False)
            sweep(odd, even, mom, False)
            return carry

        sweep(q0, even, m0, True)
        lax.fori_loop(0, 3, pair, 0)
        sweep(even, odd, mom, False)
        first = 8 * base - 8
        settle(joined(odd[pl.ds(16 + first, 32), :]), [(0, 32, first)])

    def inner_last(odd, mom, first, sums):
        return lax.fori_loop(first, first + 4, lambda i, sums: finish(odd, i, mom, i, i, sums), sums)

    inner(qm_0, qm_1, pm, 7)

    def to_column(src, tab, send_sem, recv_sem):
        for k in range(8):
            push(src, tab.at[place], send_sem, recv_sem, join_rep(x, (z + k) % 8, y, c))

    def to_plane(tab, dst, send_sem, recv_sem):
        block = pl.ds(pl.multiple_of(group * 8, 8), 8)
        for k in range(16):
            push(
                tab.at[block], dst.at[block], send_sem, recv_sem,
                join_rep((x + k // 4) % 4, z, (y + (k // 2) % 2) % 2, (c + k % 2) % 2),
            )

    def each(start, finish_part=None):
        def one(n, carry):
            part = lax.rem(part_of_me + n, 8)
            for k in range(16):
                start(part, turned[k], part * 16 + turned[k])
                if finish_part is not None and k % 4 == 3:
                    finish_part(n, k // 4)
            return carry

        lax.fori_loop(0, 8, one, 0)

    def spread(chunk, beside=None):
        mine = got[chunk].at[me]

        def start(part, at, home):
            push(half_tile(out_ref, chunk, part, at), mine, send_1.at[chunk], recv_1.at[chunk], home)

        each(start, beside)

    def pick(chunk):
        def one(t, carry):
            picked[chunk][t] = got[chunk][holder_ref[0, t]]
            return carry

        lax.fori_loop(0, 128, one, 0, unroll=8)

    def give(chunk):
        mine = half_tile(sorted_ref, chunk, part_of_me, lane_of_me)

        def start(part, at, goal):
            push(picked[chunk].at[goal], mine, send_2.at[chunk], recv_2, goal)

        each(start)

    halos = ((q0, 136, 8), (q0, 16, 144), (m0, 136, 8), (m0, 16, 144))
    edges = ((q0, 135, 7), (q0, 24, 152))

    def halo(n, k):
        ref, src_row, dst_row = halos[k]
        cols = pl.ds(pl.multiple_of(256 * n, 128), 256)
        push(
            ref.at[pl.ds(src_row, 8), cols], ref.at[pl.ds(dst_row, 8), cols],
            send_h.at[k], recv_h.at[k], me,
        )

    pl.semaphore_wait(barrier, 128)
    to_column(label_row, label_tab.at[0], send_lab.at[0], recv_lab.at[0])
    spread(0)

    loads[2].wait()
    loads[3].wait()
    set_apart(0, 1)
    inner(qa_0, qa_1, pa, 3)
    wait_for(label_tab.at[0, pl.ds(0, 8)], recv_lab.at[0])
    to_plane(label_tab.at[0], label_tab.at[1], send_lab.at[1], recv_lab.at[1])
    spread(1)

    loads[4].wait()
    loads[5].wait()
    set_apart(3, 1)
    inner(qa_0, qa_1, pa, 11)
    for k, (ref, src_row, dst_row) in enumerate(edges):
        push(ref.at[pl.ds(src_row, 1)], ref.at[pl.ds(dst_row, 1)], send_h.at[4 + k], recv_h.at[4 + k], me)
    spread(2, halo)

    lane = lax.broadcasted_iota(jnp.int32, (1, 128), 1)
    wait_for(label_tab.at[1], recv_lab.at[1])
    holder = jnp.zeros((1, 128), jnp.int32)
    for p in range(128):
        rep = join_rep(p // 32, p % 8, (p // 16) % 2, (p // 8) % 2)
        holder = jnp.maximum(holder, jnp.where(label_tab[1, p] == lane, rep, 0))
    holder_row[...] = holder
    copy = pltpu.make_async_copy(holder_row, holder_ref, local_sem)
    copy.start()
    copy.wait()

    wait_for(got_0, recv_1.at[0])
    pick(0)
    give(0)
    wait_for(got_1, recv_1.at[1])
    pick(1)
    give(1)

    for k, (ref, src_row, dst_row) in enumerate(halos):
        wait_for(ref.at[pl.ds(dst_row, 8)], recv_h.at[k])
    for k, (ref, src_row, dst_row) in enumerate(edges):
        wait_for(ref.at[pl.ds(dst_row, 1)], recv_h.at[4 + k])

    def outer(src, dst, mom, first):
        def some(side, carry):
            for k in range(1, 5):
                at = (14 if first else 6) * side + k
                leap(src, at, mom, at, dst, pe, 6 * side + k, first)
            return carry

        lax.fori_loop(0, 2, some, 0)

    def outer_pair(n, carry):
        outer(qe_0, qe_1, pe, False)
        outer(qe_1, qe_0, pe, False)
        return carry

    outer(q0, qe_0, m0, True)
    lax.fori_loop(0, 3, outer_pair, 0)
    outer(qe_0, qe_1, pe, False)
    settle(
        joined(jnp.concatenate((qe_1[pl.ds(16, 16), :], qe_1[pl.ds(64, 16), :]), 0)),
        [(0, 16, 0), (16, 16, 112)],
    )
    spread(3)

    def outer_last(i, sums):
        side, local = lax.div(i, 2), 2 + lax.rem(i, 2)
        return finish(qe_1, 6 * side + local, pe, 6 * side + local, 14 * side + local, sums)

    zero = jnp.zeros((8, 128), F32)
    sums = lax.fori_loop(0, 4, outer_last, (zero, zero))
    sums = inner_last(qm_1, pm, 8, sums)
    sums = inner_last(qa_1, pa, 4, sums)
    sums = inner_last(qa_1, pa, 12, sums)
    act_row[...] = jnp.where(lane == 0, jnp.sum(sums[1]), jnp.where(lane == 1, jnp.sum(sums[0]), 0.0))
    push(act_row, act_got, send_act.at[0], recv_act.at[0], me)

    wait_for(got_2, recv_1.at[2])
    pick(2)
    give(2)
    wait_for(act_got, recv_act.at[0])
    total = act_row[...] + act_got[...]
    act_sum[...] = total
    to_column(act_sum, act_tab.at[0], send_act.at[1], recv_act.at[1])
    wait_for(got_3, recv_1.at[3])
    pick(3)
    wait_for(act_tab.at[0, pl.ds(0, 8)], recv_act.at[1])
    to_plane(act_tab.at[0], act_tab.at[1], send_act.at[2], recv_act.at[2])
    give(3)

    for k, (ref, src_row, dst_row) in enumerate(halos):
        wait_for(ref.at[pl.ds(src_row, 8)], send_h.at[k])
    for k, (ref, src_row, dst_row) in enumerate(edges):
        wait_for(ref.at[pl.ds(src_row, 1)], send_h.at[4 + k])
    wait_for(label_tab.at[0, pl.ds(0, 8)], send_lab.at[0])
    wait_for(label_tab.at[1], send_lab.at[1])
    wait_for(act_got, send_act.at[0])
    wait_for(act_tab.at[0, pl.ds(0, 8)], send_act.at[1])
    for chunk in range(CHUNKS):
        wait_for(got[chunk], send_1.at[chunk])
    wait_for(act_tab.at[1], recv_act.at[2])
    ladder = jnp.zeros((1, 128), F32)
    for p in range(128):
        ladder = ladder + jnp.where(label_tab[1, p] == me, act_tab[1, p], 0.0)
    act_out[...] = jnp.where(lane == 0, ladder / 524288.0, total)
    wait_for(act_tab.at[1], send_act.at[2])
    for chunk in range(CHUNKS):
        wait_for(got[chunk], send_2.at[chunk])
    wait_for(sorted_ref, recv_2)


def hand_over(out_in, sorted_in, label_in, act_in, out, ordered, new, change, ladder, new_s, change_s, ladder_s, sems):
    copies = [pltpu.make_async_copy(out_in, out, sems.at[0]), pltpu.make_async_copy(sorted_in, ordered, sems.at[1])]
    for copy in copies:
        copy.start()
    lane = lax.broadcasted_iota(jnp.int32, (1, 128), 1)
    new_s[0] = jnp.max(label_in[...])
    change_s[0] = jnp.sum(jnp.where(lane == 1, act_in[...], 0.0))
    ladder_s[0] = jnp.sum(jnp.where(lane == 0, act_in[...], 0.0))
    for k, (src, dst) in enumerate(((new_s, new), (change_s, change), (ladder_s, ladder))):
        copies.append(pltpu.make_async_copy(src, dst, sems.at[2 + k]))
        copies[-1].start()
    for copy in copies:
        copy.wait()


def body(field, momentum, labels, betas, accept, swap_pairs):
    i32 = jnp.int32
    dma = pltpu.SemaphoreType.DMA
    strip = jax.ShapeDtypeStruct((16, 8, 2048), F32)
    hbm = pl.BlockSpec(memory_space=pltpu.HBM)
    vmem = pl.BlockSpec(memory_space=pltpu.VMEM)
    shapes = (
        strip, strip, jax.ShapeDtypeStruct((1,), i32),
        jax.ShapeDtypeStruct((1,), F32), jax.ShapeDtypeStruct((1,), F32),
    )
    smalls = (jax.ShapeDtypeStruct((1, 128), i32), jax.ShapeDtypeStruct((1, 128), F32))
    results = pl.pallas_call(
        whole,
        out_shape=(strip, strip, *smalls),
        in_specs=[hbm] * 6,
        out_specs=(vmem,) * 4,
        scratch_shapes=[
            pltpu.SMEM((1,), i32),
            pltpu.SMEM((128,), F32),
            pltpu.SMEM((1,), i32),
            pltpu.SMEM((128,), i32),
            pltpu.VMEM((128, 2048), F32),
            pltpu.VMEM((128, 2048), F32),
            pltpu.VMEM((160, 2048), F32),
            pltpu.VMEM((160, 2048), F32),
            pltpu.VMEM((160, 2048), F32),
            pltpu.VMEM((160, 2048), F32),
            pltpu.VMEM((160, 2048), F32),
            pltpu.VMEM((160, 2048), F32),
            pltpu.VMEM((160, 2048), F32),
            pltpu.VMEM((160, 2048), F32),
            pltpu.VMEM((96, 2048), F32),
            pltpu.VMEM((96, 2048), F32),
            pltpu.VMEM((96, 2048), F32),
            pltpu.VMEM((768, 256), BF16),
            pltpu.VMEM((512, 256), BF16),
            *[pltpu.VMEM((128, 4, 128), F32)] * 8,
            pltpu.VMEM((1, 128), i32),
            pltpu.VMEM((2, 128, 1, 128), i32),
            pltpu.VMEM((1, 128), F32),
            pltpu.VMEM((1, 128), F32),
            pltpu.VMEM((1, 128), F32),
            pltpu.VMEM((2, 128, 1, 128), F32),
            pltpu.VMEM((1, 128), i32),
            pltpu.SMEM((1, 128), i32),
            dma((6,)), dma((6,)), dma((4,)), dma((4,)), dma((4,)), dma(()),
            dma((2,)), dma((2,)), dma((3,)), dma((3,)), dma(()), dma((6,)), dma((4,)),
        ],
        compiler_params=pltpu.CompilerParams(collective_id=0, has_side_effects=True, vmem_limit_bytes=53_500_000),
    )(field, momentum, labels, betas, accept, swap_pairs)
    out, ordered, new_label, change, ladder = pl.pallas_call(
        hand_over,
        out_shape=shapes,
        in_specs=[vmem] * 4,
        out_specs=(hbm,) * 5,
        scratch_shapes=[pltpu.SMEM((1,), i32), pltpu.SMEM((1,), F32), pltpu.SMEM((1,), F32), dma((5,))],
        compiler_params=pltpu.CompilerParams(vmem_limit_bytes=8 << 20),
    )(*results)
    return out.reshape(1, 128, 2048), ordered.reshape(1, 128, 2048), new_label, change, ladder


def solution(mesh):
    rep = P("rep")
    strip = P("rep", "dom", None)
    in_specs = (strip, strip, rep, P(), rep, P())
    out_specs = (strip, strip, rep, rep, rep)
    return jax.shard_map(body, mesh=mesh, in_specs=in_specs, out_specs=out_specs, check_vma=False)
```

```python
import functools
import jax
import jax.numpy as jnp
from jax import lax
from jax.experimental import pallas as pl
from jax.experimental.pallas import tpu as pltpu
from jax.sharding import PartitionSpec as P

MESH = pl.DeviceIdType.MESH

HOP = 0.36
QUARTIC = 0.3
EPS = 0.05
F32 = jnp.float32
BF16 = jnp.bfloat16

def split_rep(rep):
    return rep // 32, (rep // 4) % 8, (rep // 2) % 2, rep % 2


def join_rep(x, z, y, c):
    return ((x * 8 + z) * 2 + y) * 2 + c


def table_place(rep):
    x, z, y, c = split_rep(rep)
    return ((x * 2 + y) * 2 + c) * 8 + z


def half_tile(ref, chunk, part, at):
    b, half = lax.div(part, 2), pl.ds(pl.multiple_of(4 * lax.rem(part, 2), 4), 4)
    block = b + 12 * lax.div(b, 2) if chunk == 3 else (6, 2, 10)[chunk] + b
    return ref.at[block, half, pl.ds(pl.multiple_of(128 * at, 128), 128)]


def wait_for(ref, sem):
    pltpu.make_async_copy(ref, ref, sem).wait()


def rows_of(block):
    return pl.ds(pl.multiple_of(block * 8, 8), 8)


def lateral(q):
    even, odd = q[:, :1024], q[:, 1024:]
    after = pltpu.roll(even, 1023, 1)
    return jnp.concatenate((odd + pltpu.roll(odd, 1, 1), even + after), 1), jnp.concatenate((odd, after), 1)


def fold(v):
    total = v[:, :128]
    for j in range(1, 16):
        total = total + v[:, 128 * j : 128 * j + 128]
    return total


def split_two(v):
    high = v.astype(BF16)
    return high, (v - high.astype(F32)).astype(BF16)


def site(q, below, right):
    squared = q * q
    return -HOP * q * (below + right) + squared + QUARTIC * (squared - 1.0) * (squared - 1.0)


CHUNKS = 4


def whole(
    field_hbm, moment_hbm, labels_hbm, betas_hbm, accept_hbm, pairs_hbm,
    out_ref, sorted_ref, label_out, act_out,
    labels_ref, betas_ref, accept_ref, pairs_ref,
    field_ref, moment_ref, q0, m0, qm_0, qm_1, pm, qa_0, qa_1, pa, qe_0, qe_1, pe, perm, perm_back,
    got_0, got_1, got_2, got_3, picked_0, picked_1, picked_2, picked_3, label_row, label_tab, act_row, act_got, act_sum, act_tab, holder_row, holder_ref,
    send_h, recv_h, send_1, recv_1, send_2, recv_2, send_lab, recv_lab, send_act, recv_act, local_sem, load_sem, small_sem,
):
    me = lax.axis_index("rep")
    dom = lax.axis_index("dom")
    other = 1 - dom
    x, z, y, c = split_rep(me)
    place = table_place(me)
    group = lax.div(place, 8)
    got = (got_0, got_1, got_2, got_3)
    picked = (picked_0, picked_1, picked_2, picked_3)
    part_of_me, lane_of_me = lax.div(me, 16), lax.rem(me, 16)
    turned = [lax.rem(lane_of_me + k, 16) for k in range(16)]

    loads = []
    for first, n in ((32, 64), (0, 32), (96, 32)):
        rows = pl.ds(first, n)
        for src, dst in ((field_hbm, field_ref), (moment_hbm, moment_ref)):
            loads.append(pltpu.make_async_copy(src.at[0, rows], dst.at[rows], load_sem.at[len(loads)]))
            loads[-1].start()
    small = []
    for k, (src, dst) in enumerate(
        ((labels_hbm, labels_ref), (betas_hbm, betas_ref), (accept_hbm, accept_ref), (pairs_hbm, pairs_ref))
    ):
        small.append(pltpu.make_async_copy(src, dst, small_sem.at[k]))
        small[k].start()

    def push(src, dst, send_sem, recv_sem, rep):
        pltpu.make_async_remote_copy(
            src_ref=src, dst_ref=dst, send_sem=send_sem, recv_sem=recv_sem,
            device_id=(rep, other), device_id_type=MESH,
        ).start()

    barrier = pltpu.get_barrier_semaphore()

    xs = [lax.rem(x + k, 4) * 32 for k in (2, 1, 3, 0)]
    zs = [lax.rem(z + k, 8) * 4 for k in (4, 3, 5, 2, 6, 1, 7, 0)]
    for at_z in zs:
        for at_x in xs:
            for k in range(4):
                pl.semaphore_signal(barrier, inc=1, device_id=(at_x + at_z + k, other), device_id_type=MESH)

    for copy in small:
        copy.wait()
    label = labels_ref[0]
    coldness = betas_ref[label]
    new_label = pairs_ref[label]
    accepted = accept_ref[0] == 1
    label_out[...] = jnp.full((1, 128), new_label, jnp.int32)
    label_row[...] = jnp.full((1, 128), new_label, jnp.int32)

    i0 = lax.broadcasted_iota(jnp.int32, (256, 256), 0)
    i1 = lax.broadcasted_iota(jnp.int32, (256, 256), 1)
    there = jnp.where(i1 < 128, 2 * i1, 2 * i1 - 255) == i0
    back = jnp.where(i0 < 128, 2 * i0, 2 * i0 - 255) == i1
    for third in range(3):
        perm[pl.ds(256 * third, 256), :] = jnp.where(there, 1.0, 0.0).astype(BF16)
    for half in range(2):
        perm_back[pl.ds(256 * half, 256), :] = jnp.where(back, 1.0, 0.0).astype(BF16)

    def apart(ref, dst, r):
        values = ref[pl.ds(pl.multiple_of(32 * r, 32), 32), :]
        high = values.astype(BF16)
        pieces = (high, *split_two(values - high.astype(F32)))
        cols = [slice(256 * b, 256 * b + 256) for b in range(8)]
        left = jnp.concatenate([jnp.concatenate([v[:, s] for v in pieces], 1) for s in cols], 0)
        res = jnp.dot(left, perm[...], preferred_element_type=F32)
        rows = pl.ds(pl.multiple_of(16 + 32 * r, 16), 32)
        for b in range(8):
            dst[rows, 128 * b : 128 * b + 128] = res[32 * b : 32 * b + 32, :128]
            dst[rows, 1024 + 128 * b : 1152 + 128 * b] = res[32 * b : 32 * b + 32, 128:]

    def joined(values):
        high, low = split_two(values)
        parts = []
        for b in range(8):
            e = slice(128 * b, 128 * b + 128)
            o = slice(1024 + 128 * b, 1152 + 128 * b)
            parts.append(jnp.concatenate((high[:, e], high[:, o], low[:, e], low[:, o]), 1))
        res = jnp.dot(jnp.concatenate(parts, 0), perm_back[...], preferred_element_type=F32)
        return jnp.concatenate([res[32 * b : 32 * b + 32] for b in range(8)], 1)

    def settle(values, rows):
        for at, n, first in rows:
            new = jnp.where(accepted, values[at : at + n], field_ref[pl.ds(first, n), :])
            out_ref[pl.ds(first // 8, n // 8)] = new.reshape(n // 8, 8, 2048)

    def set_apart(first, count):
        def one(n, carry):
            apart(field_ref, q0, first + n)
            apart(moment_ref, m0, first + n)
            return carry

        lax.fori_loop(0, count, one, 0)

    loads[0].wait()
    loads[1].wait()
    set_apart(1, 2)

    row = lax.broadcasted_iota(jnp.int32, (8, 2048), 0)
    a = coldness * (EPS * HOP)
    b = coldness * (EPS * (2.0 - 4.0 * QUARTIC))
    g = coldness * (EPS * 4.0 * QUARTIC)

    def around(ref, block):
        q = ref[rows_of(block), :]
        above = pltpu.roll(jnp.where(row == 7, ref[rows_of(block - 1), :], q), 1, 0)
        below = pltpu.roll(jnp.where(row == 0, ref[rows_of(block + 1), :], q), 7, 0)
        return q, above, below

    def kicked(q, above, below, beside, moment, share):
        near = (above + below) + beside
        return moment + (near * (share * a) - q * (q * q * (share * g) + share * b))

    def leap(src, src_at, mom, mom_at, dst, dst_p, at, first):
        q, above, below = around(src, src_at)
        beside, _ = lateral(q)
        moment = mom[rows_of(mom_at), :]
        moment = kicked(q, above, below, beside, moment, 0.5 if first else 1.0)
        dst_p[rows_of(at), :] = moment
        dst[rows_of(at), :] = q + EPS * moment

    def finish(src, src_at, mom, mom_at, start_at, sums):
        q, above, below = around(src, src_at)
        beside, right = lateral(q)
        moment = kicked(q, above, below, beside, mom[rows_of(mom_at), :], 0.5)
        new = site(q, below, right)
        p, _, p_below = around(q0, start_at)
        old = site(p, p_below, lateral(p)[1])
        start = m0[rows_of(start_at), :]
        change = (0.5 * moment * moment + coldness * new) - (0.5 * start * start + coldness * old)
        return sums[0] + fold(change), sums[1] + fold(jnp.where(accepted, new, old))

    def inner(even, odd, mom, base):
        def sweep(src, dst, src_p, first):
            for at in range(base, base + 6):
                leap(src, at, src_p, at, dst, mom, at, first)

        def pair(n, carry):
            sweep(even, odd, mom, False)
            sweep(odd, even, mom, False)
            return carry

        sweep(q0, even, m0, True)
        lax.fori_loop(0, 3, pair, 0)
        sweep(even, odd, mom, False)
        first = 8 * base - 8
        settle(joined(odd[pl.ds(16 + first, 32), :]), [(0, 32, first)])

    def inner_last(odd, mom, first, sums):
        return lax.fori_loop(first, first + 4, lambda i, sums: finish(odd, i, mom, i, i, sums), sums)

    inner(qm_0, qm_1, pm, 7)

    def to_column(src, tab, send_sem, recv_sem):
        for k in range(8):
            push(src, tab.at[place], send_sem, recv_sem, join_rep(x, (z + k) % 8, y, c))

    def to_plane(tab, dst, send_sem, recv_sem):
        block = pl.ds(pl.multiple_of(group * 8, 8), 8)
        for k in range(16):
            push(
                tab.at[block], dst.at[block], send_sem, recv_sem,
                join_rep((x + k // 4) % 4, z, (y + (k // 2) % 2) % 2, (c + k % 2) % 2),
            )

    def each(start, finish_part=None):
        def one(n, carry):
            part = lax.rem(part_of_me + n, 8)
            for k in range(16):
                start(part, turned[k], part * 16 + turned[k])
                if finish_part is not None and k % 4 == 3:
                    finish_part(n, k // 4)
            return carry

        lax.fori_loop(0, 8, one, 0)

    def spread(chunk, beside=None):
        mine = got[chunk].at[me]

        def start(part, at, home):
            push(half_tile(out_ref, chunk, part, at), mine, send_1.at[chunk], recv_1.at[chunk], home)

        each(start, beside)

    def pick(chunk):
        def one(t, carry):
            picked[chunk][t] = got[chunk][holder_ref[0, t]]
            return carry

        lax.fori_loop(0, 128, one, 0, unroll=8)

    def give(chunk):
        mine = half_tile(sorted_ref, chunk, part_of_me, lane_of_me)

        def start(part, at, goal):
            push(picked[chunk].at[goal], mine, send_2.at[chunk], recv_2, goal)

        each(start)

    halos = ((q0, 136, 8), (q0, 16, 144), (m0, 136, 8), (m0, 16, 144))
    edges = ((q0, 135, 7), (q0, 24, 152))

    def halo(n, k):
        ref, src_row, dst_row = halos[k]
        cols = pl.ds(pl.multiple_of(256 * n, 128), 256)
        push(
            ref.at[pl.ds(src_row, 8), cols], ref.at[pl.ds(dst_row, 8), cols],
            send_h.at[k], recv_h.at[k], me,
        )

    pl.semaphore_wait(barrier, 128)
    to_column(label_row, label_tab.at[0], send_lab.at[0], recv_lab.at[0])
    spread(0)

    loads[2].wait()
    loads[3].wait()
    set_apart(0, 1)
    inner(qa_0, qa_1, pa, 3)
    wait_for(label_tab.at[0, pl.ds(0, 8)], recv_lab.at[0])
    to_plane(label_tab.at[0], label_tab.at[1], send_lab.at[1], recv_lab.at[1])
    spread(1)

    loads[4].wait()
    loads[5].wait()
    set_apart(3, 1)
    inner(qa_0, qa_1, pa, 11)
    for k, (ref, src_row, dst_row) in enumerate(edges):
        push(ref.at[pl.ds(src_row, 1)], ref.at[pl.ds(dst_row, 1)], send_h.at[4 + k], recv_h.at[4 + k], me)
    spread(2, halo)

    lane = lax.broadcasted_iota(jnp.int32, (1, 128), 1)
    wait_for(label_tab.at[1], recv_lab.at[1])
    holder = jnp.zeros((1, 128), jnp.int32)
    for p in range(128):
        rep = join_rep(p // 32, p % 8, (p // 16) % 2, (p // 8) % 2)
        holder = jnp.maximum(holder, jnp.where(label_tab[1, p] == lane, rep, 0))
    holder_row[...] = holder
    copy = pltpu.make_async_copy(holder_row, holder_ref, local_sem)
    copy.start()
    copy.wait()

    wait_for(got_0, recv_1.at[0])
    pick(0)
    give(0)
    zero = jnp.zeros((8, 128), F32)
    sums = inner_last(qm_1, pm, 8, (zero, zero))
    sums = inner_last(qa_1, pa, 4, sums)
    sums = inner_last(qa_1, pa, 12, sums)
    wait_for(got_1, recv_1.at[1])
    pick(1)
    give(1)

    for k, (ref, src_row, dst_row) in enumerate(halos):
        wait_for(ref.at[pl.ds(dst_row, 8)], recv_h.at[k])
    for k, (ref, src_row, dst_row) in enumerate(edges):
        wait_for(ref.at[pl.ds(dst_row, 1)], recv_h.at[4 + k])

    def outer(src, dst, mom, first):
        def some(side, carry):
            for k in range(1, 5):
                at = (14 if first else 6) * side + k
                leap(src, at, mom, at, dst, pe, 6 * side + k, first)
            return carry

        lax.fori_loop(0, 2, some, 0)

    def outer_pair(n, carry):
        outer(qe_0, qe_1, pe, False)
        outer(qe_1, qe_0, pe, False)
        return carry

    outer(q0, qe_0, m0, True)
    lax.fori_loop(0, 3, outer_pair, 0)
    outer(qe_0, qe_1, pe, False)
    settle(
        joined(jnp.concatenate((qe_1[pl.ds(16, 16), :], qe_1[pl.ds(64, 16), :]), 0)),
        [(0, 16, 0), (16, 16, 112)],
    )
    spread(3)

    def outer_last(i, sums):
        side, local = lax.div(i, 2), 2 + lax.rem(i, 2)
        return finish(qe_1, 6 * side + local, pe, 6 * side + local, 14 * side + local, sums)

    sums = lax.fori_loop(0, 4, outer_last, sums)
    act_row[...] = jnp.where(lane == 0, jnp.sum(sums[1]), jnp.where(lane == 1, jnp.sum(sums[0]), 0.0))
    push(act_row, act_got, send_act.at[0], recv_act.at[0], me)

    wait_for(got_2, recv_1.at[2])
    pick(2)
    give(2)
    wait_for(act_got, recv_act.at[0])
    total = act_row[...] + act_got[...]
    act_sum[...] = total
    to_column(act_sum, act_tab.at[0], send_act.at[1], recv_act.at[1])
    wait_for(got_3, recv_1.at[3])
    pick(3)
    wait_for(act_tab.at[0, pl.ds(0, 8)], recv_act.at[1])
    to_plane(act_tab.at[0], act_tab.at[1], send_act.at[2], recv_act.at[2])
    give(3)

    for k, (ref, src_row, dst_row) in enumerate(halos):
        wait_for(ref.at[pl.ds(src_row, 8)], send_h.at[k])
    for k, (ref, src_row, dst_row) in enumerate(edges):
        wait_for(ref.at[pl.ds(src_row, 1)], send_h.at[4 + k])
    wait_for(label_tab.at[0, pl.ds(0, 8)], send_lab.at[0])
    wait_for(label_tab.at[1], send_lab.at[1])
    wait_for(act_got, send_act.at[0])
    wait_for(act_tab.at[0, pl.ds(0, 8)], send_act.at[1])
    for chunk in range(CHUNKS):
        wait_for(got[chunk], send_1.at[chunk])
    wait_for(act_tab.at[1], recv_act.at[2])
    ladder = jnp.zeros((1, 128), F32)
    for p in range(128):
        ladder = ladder + jnp.where(label_tab[1, p] == me, act_tab[1, p], 0.0)
    act_out[...] = jnp.where(lane == 0, ladder / 524288.0, total)
    wait_for(act_tab.at[1], send_act.at[2])
    for chunk in range(CHUNKS):
        wait_for(got[chunk], send_2.at[chunk])
    wait_for(sorted_ref, recv_2)


def hand_over(out_in, sorted_in, label_in, act_in, out, ordered, new, change, ladder, new_s, change_s, ladder_s, sems):
    copies = [pltpu.make_async_copy(out_in, out, sems.at[0]), pltpu.make_async_copy(sorted_in, ordered, sems.at[1])]
    for copy in copies:
        copy.start()
    lane = lax.broadcasted_iota(jnp.int32, (1, 128), 1)
    new_s[0] = jnp.max(label_in[...])
    change_s[0] = jnp.sum(jnp.where(lane == 1, act_in[...], 0.0))
    ladder_s[0] = jnp.sum(jnp.where(lane == 0, act_in[...], 0.0))
    for k, (src, dst) in enumerate(((new_s, new), (change_s, change), (ladder_s, ladder))):
        copies.append(pltpu.make_async_copy(src, dst, sems.at[2 + k]))
        copies[-1].start()
    for copy in copies:
        copy.wait()


def body(field, momentum, labels, betas, accept, swap_pairs):
    i32 = jnp.int32
    dma = pltpu.SemaphoreType.DMA
    strip = jax.ShapeDtypeStruct((16, 8, 2048), F32)
    hbm = pl.BlockSpec(memory_space=pltpu.HBM)
    vmem = pl.BlockSpec(memory_space=pltpu.VMEM)
    shapes = (
        strip, strip, jax.ShapeDtypeStruct((1,), i32),
        jax.ShapeDtypeStruct((1,), F32), jax.ShapeDtypeStruct((1,), F32),
    )
    smalls = (jax.ShapeDtypeStruct((1, 128), i32), jax.ShapeDtypeStruct((1, 128), F32))
    results = pl.pallas_call(
        whole,
        out_shape=(strip, strip, *smalls),
        in_specs=[hbm] * 6,
        out_specs=(vmem,) * 4,
        scratch_shapes=[
            pltpu.SMEM((1,), i32),
            pltpu.SMEM((128,), F32),
            pltpu.SMEM((1,), i32),
            pltpu.SMEM((128,), i32),
            pltpu.VMEM((128, 2048), F32),
            pltpu.VMEM((128, 2048), F32),
            pltpu.VMEM((160, 2048), F32),
            pltpu.VMEM((160, 2048), F32),
            pltpu.VMEM((160, 2048), F32),
            pltpu.VMEM((160, 2048), F32),
            pltpu.VMEM((160, 2048), F32),
            pltpu.VMEM((160, 2048), F32),
            pltpu.VMEM((160, 2048), F32),
            pltpu.VMEM((160, 2048), F32),
            pltpu.VMEM((96, 2048), F32),
            pltpu.VMEM((96, 2048), F32),
            pltpu.VMEM((96, 2048), F32),
            pltpu.VMEM((768, 256), BF16),
            pltpu.VMEM((512, 256), BF16),
            *[pltpu.VMEM((128, 4, 128), F32)] * 8,
            pltpu.VMEM((1, 128), i32),
            pltpu.VMEM((2, 128, 1, 128), i32),
            pltpu.VMEM((1, 128), F32),
            pltpu.VMEM((1, 128), F32),
            pltpu.VMEM((1, 128), F32),
            pltpu.VMEM((2, 128, 1, 128), F32),
            pltpu.VMEM((1, 128), i32),
            pltpu.SMEM((1, 128), i32),
            dma((6,)), dma((6,)), dma((4,)), dma((4,)), dma((4,)), dma(()),
            dma((2,)), dma((2,)), dma((3,)), dma((3,)), dma(()), dma((6,)), dma((4,)),
        ],
        compiler_params=pltpu.CompilerParams(collective_id=0, has_side_effects=True, vmem_limit_bytes=53_500_000),
    )(field, momentum, labels, betas, accept, swap_pairs)
    out, ordered, new_label, change, ladder = pl.pallas_call(
        hand_over,
        out_shape=shapes,
        in_specs=[vmem] * 4,
        out_specs=(hbm,) * 5,
        scratch_shapes=[pltpu.SMEM((1,), i32), pltpu.SMEM((1,), F32), pltpu.SMEM((1,), F32), dma((5,))],
        compiler_params=pltpu.CompilerParams(vmem_limit_bytes=8 << 20),
    )(*results)
    return out.reshape(1, 128, 2048), ordered.reshape(1, 128, 2048), new_label, change, ladder


def solution(mesh):
    rep = P("rep")
    strip = P("rep", "dom", None)
    in_specs = (strip, strip, rep, P(), rep, P())
    out_specs = (strip, strip, rep, rep, rep)
    return jax.shard_map(body, mesh=mesh, in_specs=in_specs, out_specs=out_specs, check_vma=False)
```
